256 devices in a mesh: seq: 16 (over y, x), width: 16 (over z, core).
Axes of the slice: x: 4, y: 4, z: 8, core: 2. Of those that a mesh axis runs over, the one named last changes fastest.
Arguments:
- leak_rate: float32 [1, 32768, 2048], P(None, 'seq', 'width'), may hold values from 0.2 to 2
- signal_in: bfloat16 [1, 32768, 2048], P(None, 'seq', 'width'), may hold values from -6 to 6
- norm_gain: float32 [2048], P('width'), may hold values from 0.25 to 1.75
Outputs:
- mixed_out: bfloat16 [1, 32768, 2048], P(None, 'seq', 'width')
The draws below stay inside these ranges and needn't reach their ends.
All inputs are finite; a program needn't handle non-finite values.
Results may differ from the reference program's by a relative error of at most 0.001.
Values sent between devices are 32-bit elements; how exact they have to be, the bound alone decides.
A program may use at most 64 MiB of HBM per device.

```python
import jax
import jax.numpy as jnp
from jax import lax

BATCH = 1
CHANNELS = 2048
LENGTH = 32768


def steps_of(own_key, dims, cuts, low, high):
    def one(position, blocks):
        heights = jax.random.uniform(jax.random.fold_in(jax.random.fold_in(own_key, 6), position), (blocks,), jnp.float32, low / len(cuts), high / len(cuts))
        return jnp.repeat(jnp.exp(heights), dims[position] // blocks).reshape((-1,) + (1,) * (len(dims) - position - 1))

    factor_of = one(*cuts[0])
    for cut in cuts[1:]:
        factor_of = factor_of * one(*cut)
    return factor_of


def bell_draw(rng, shape, scale, limit, shards=(), held_as=jnp.bfloat16):
    loudness = steps_of(rng, shape, shards, -0.22, 0.18) if shards else 1.0
    drawn = jax.random.normal(rng, shape, jnp.float32) * scale * loudness
    return jnp.minimum(jnp.maximum(drawn, -limit), limit).astype(held_as)


def setup_inputs(seed: int = 0) -> dict:
    seeds = jax.random.split(jax.random.key(seed), 4)
    leak_rate = jnp.clip(0.2 + 1.8 * jax.random.uniform(seeds[0], (BATCH, LENGTH, CHANNELS), jnp.float32) ** steps_of(seeds[0], (BATCH, LENGTH, CHANNELS), ((1, 16), (2, 16)), -0.2, 0.2), 0.2, 2.0)
    signal_in = bell_draw(seeds[1], (BATCH, LENGTH, CHANNELS), 1.0, 6.0, ((1, 16), (2, 16)))
    norm_gain = jnp.clip(1.0 + 0.15 * jax.random.normal(seeds[2], (CHANNELS,), jnp.float32), 0.25, 1.75)
    return {"leak_rate": leak_rate, "signal_in": signal_in, "norm_gain": norm_gain}


def join_pair(earlier, later):
    return (earlier[0] * later[0], later[0] * earlier[1] + later[1])

def reference(leak_rate, signal_in, norm_gain):
    keep = jnp.exp(-leak_rate / LENGTH)
    push = signal_in.astype(jnp.float32) * LENGTH ** (-0.5)
    forward = lax.associative_scan(join_pair, (keep, push), axis=1)[1]
    backward = lax.associative_scan(join_pair, (keep, push), axis=1, reverse=True)[1]
    states = forward + backward
    power = lax.optimization_barrier(jnp.mean(states * states, axis=-1, keepdims=True))
    mixed_out = (states * lax.rsqrt(power + 1e-06) * norm_gain).astype(jnp.bfloat16)
    return mixed_out
```

```python
import functools

import jax
import jax.numpy as jnp
from jax import lax
from jax.experimental import pallas as pl
from jax.experimental.pallas import tpu as pltpu
from jax.sharding import PartitionSpec as P

LANES = 128
SUB = 8
MESH = pl.DeviceIdType.MESH


def join_kernel(ns, nw, seg, leak_hbm, sig_hbm, gain_hbm, out_v, gain_ref, state_v, wide_v, leak_v, sig_v, keep_v, push_v,
                local_v, pre_v, suf_v, tot_v, pow_v, in_sem, gain_sem, ts_sem, tr_sem, ps_sem, pr_sem):
    T, C = leak_v.shape
    G = C // LANES
    NS = T // seg
    NO = NS // SUB
    pitch = seg + 4
    rows = SUB * seg
    nb = rows // LANES
    total = T * ns
    me = lax.axis_index("seq")
    mw = lax.axis_index("width")

    def load(o):
        r = pl.ds(o * rows, rows)
        return (pltpu.make_async_copy(leak_hbm.at[r], leak_v.at[r], in_sem.at[0, o]),
                pltpu.make_async_copy(sig_hbm.at[r], sig_v.at[r], in_sem.at[1, o]))

    for o in range(NO):
        for c in load(o):
            c.start()

    gain_copy = pltpu.make_async_copy(gain_hbm, gain_ref, gain_sem)
    gain_copy.start()

    barrier = pltpu.get_barrier_semaphore()
    for k in range(1, ns):
        pl.semaphore_signal(barrier, inc=1, device_id={"seq": lax.rem(me + k, ns)}, device_id_type=MESH)
    for k in range(1, nw):
        pl.semaphore_signal(barrier, inc=1, device_id={"width": lax.rem(mw + k, nw)}, device_id_type=MESH)

    def at(o, i):
        return pl.ds(o * SUB * pitch + i, SUB, stride=pitch)

    def row_of(o, i):
        return pl.ds(pl.multiple_of((o * (seg + 1) + i) * SUB, SUB), SUB)

    zero = jnp.zeros((SUB, LANES), jnp.float32)
    one = jnp.ones((SUB, LANES), jnp.float32)

    def fill_octet(o):
        for c in load(o):
            c.wait()

        def fill(h, _):
            base = (o * (SUB // 2) + h)
            src = pl.multiple_of(base * 2 * seg, 2 * seg)
            dst = pl.multiple_of(base * 2 * pitch, SUB)
            for half in range(2):
                for j in range(0, seg, 16):
                    lk = leak_v[pl.ds(src + half * seg + j, 16), :]
                    kp = jnp.exp(lk * (-1.0 / total))
                    ps = sig_v[pl.ds(src + half * seg + j, 16), :].astype(jnp.float32) * (total ** -0.5)
                    for g in range(G):
                        cols = slice(g * LANES, (g + 1) * LANES)
                        for q in range(2):
                            to = pl.ds(dst + half * pitch + j + q * SUB, SUB)
                            keep_v[g, to, :] = kp[q * SUB:(q + 1) * SUB, cols]
                            push_v[g, to, :] = ps[q * SUB:(q + 1) * SUB, cols]
            return 0

        lax.fori_loop(0, SUB // 2, fill, 0)

    def segment_ends(octets):
        some = [(g, o) for g in range(G) for o in octets]

        def ends_step(i, carry):
            new = []
            for (g, o), (f, b, p) in zip(some, carry):
                k = keep_v.at[g][at(o, i), :]
                x = push_v.at[g][at(o, i), :]
                new.append((k * f + x, b + p * x, p * k))
            return tuple(new)

        return dict(zip(some, lax.fori_loop(0, seg, ends_step, tuple((zero, zero, one) for _ in some), unroll=8)))

    chains = [(g, o) for g in range(G) for o in range(NO)]
    ends = {}
    for octets in (range(NO // 2), range(NO // 2, NO)):
        for o in octets:
            fill_octet(o)
        ends.update(segment_ends(octets))

    def gathered(which):
        return jnp.concatenate(
            [jnp.concatenate([ends[g, o][which] for o in range(NO)], 0) for g in range(G)], 1)

    f_end, b_end, p_end = gathered(0), gathered(1), gathered(2)
    row = lax.broadcasted_iota(jnp.int32, (NS, C), 0)

    def shifted(x, d, fill):
        if d > 0:
            return jnp.where(row >= d, pltpu.roll(x, d, 0), fill)
        return jnp.where(row < NS + d, pltpu.roll(x, NS + d, 0), fill)

    pf, ff = p_end, f_end
    pb, bb = p_end, b_end
    d = 1
    while d < NS:
        ff = ff + pf * shifted(ff, d, 0.0)
        pf = pf * shifted(pf, d, 1.0)
        bb = bb + pb * shifted(bb, -d, 0.0)
        pb = pb * shifted(pb, -d, 1.0)
        d *= 2
    tot_v[me] = jnp.concatenate(
        [pf[NS - 1:NS], ff[NS - 1:NS], bb[0:1], jnp.zeros((1, C), jnp.float32)], 0)

    pl.semaphore_wait(barrier, ns + nw - 2)

    def other(k, own):
        return k + jnp.where(k >= own, 1, 0)

    def tot_send(k):
        return pltpu.make_async_remote_copy(
            src_ref=tot_v.at[me], dst_ref=tot_v.at[me], send_sem=ts_sem.at[k], recv_sem=tr_sem.at[me],
            device_id={"seq": other(k, me)}, device_id_type=MESH)

    def tot_recv(k):
        s = other(k, me)
        return pltpu.make_async_remote_copy(
            src_ref=tot_v.at[s], dst_ref=tot_v.at[s], send_sem=ts_sem.at[k], recv_sem=tr_sem.at[s],
            device_id={"seq": s}, device_id_type=MESH)

    for k in range(ns - 1):
        tot_send(k).start()

    def ahead(i, carry):
        new = []
        for (g, o), (f, p) in zip(chains, carry):
            k = keep_v.at[g][at(o, i), :]
            x = push_v.at[g][at(o, i), :]
            f = k * f + x
            p = p * k
            local_v[g, row_of(o, i), :] = f
            pre_v[g, row_of(o, i), :] = p
            new.append((f, p))
        return tuple(new)

    lax.fori_loop(0, seg, ahead, tuple((zero, one) for _ in chains), unroll=4)

    def back(n, carry):
        i = seg - 1 - n
        new = []
        for (g, o), (b, q) in zip(chains, carry):
            k = keep_v.at[g][at(o, i), :]
            x = push_v.at[g][at(o, i), :]
            b = k * b + x
            q = k * q
            r = row_of(o, i)
            local_v[g, r, :] = local_v[g, r, :] + b
            suf_v[g, r, :] = q
            new.append((b, q))
        return tuple(new)

    lax.fori_loop(0, seg, back, tuple((zero, one) for _ in chains), unroll=4)

    for k in range(ns - 1):
        tot_recv(k).wait_recv()
    f_in = jnp.zeros((1, C), jnp.float32)
    b_in = jnp.zeros((1, C), jnp.float32)
    for j in range(ns):
        t = tot_v[j]
        f_in = jnp.where(j < me, t[0:1] * f_in + t[1:2], f_in)
        t = tot_v[ns - 1 - j]
        b_in = jnp.where(ns - 1 - j > me, t[0:1] * b_in + t[2:3], b_in)
    f_in = shifted(ff, 1, 0.0) + shifted(pf, 1, 1.0) * f_in
    b_in = shifted(bb, -1, 0.0) + shifted(pb, -1, 1.0) * b_in

    ones = jnp.ones((SUB, LANES), jnp.bfloat16)
    nt = (((1,), (1,)), ((), ()))

    def flipped(w):
        return w + 1 - 2 * lax.rem(w, 2)

    def pow_send(k, o):
        return pltpu.make_async_remote_copy(
            src_ref=pow_v.at[mw, o], dst_ref=pow_v.at[mw, o], send_sem=ps_sem.at[k, o], recv_sem=pr_sem.at[mw, o],
            device_id={"width": flipped(other(k, flipped(mw)))}, device_id_type=MESH)

    def pow_recv(k, o):
        w = other(k, mw)
        return pltpu.make_async_remote_copy(
            src_ref=pow_v.at[w, o], dst_ref=pow_v.at[w, o], send_sem=ps_sem.at[k, o], recv_sem=pr_sem.at[w, o],
            device_id={"width": w}, device_id_type=MESH)

    steps = LANES // SUB
    pending = []

    def store_power(b, res):
        o, n = divmod(b, nb)
        pow_v[mw, o, pl.ds(n, 1), :] = res[0:1]
        if n == nb - 1:
            for k in range(nw - 1):
                pow_send(k, o).start()

    for b in range(NO * nb):
        o, n = divmod(b, nb)
        sq = []
        for i in range(n * steps, (n + 1) * steps):
            x = None
            r = pl.ds((o * (seg + 1) + i) * SUB, SUB)
            for g in range(G):
                c = slice(g * LANES, (g + 1) * LANES)
                st = (local_v[g, r, :] + pre_v[g, r, :] * f_in[o * SUB:(o + 1) * SUB, c]
                      + suf_v[g, r, :] * b_in[o * SUB:(o + 1) * SUB, c])
                state_v.at[g][at(o, i), :] = st
                x = st * st if x is None else x + st * st
            sq.append(x)
        x = jnp.concatenate(sq, 0)
        hi = x.astype(jnp.bfloat16)
        lo = (x - hi.astype(jnp.float32)).astype(jnp.bfloat16)
        pending.append((b, lax.dot_general(ones, hi, nt, preferred_element_type=jnp.float32)
                        + lax.dot_general(ones, lo, nt, preferred_element_type=jnp.float32)))
        if len(pending) > 2:
            store_power(*pending.pop(0))
    for p in pending:
        store_power(*p)

    gain_copy.wait()
    gain = gain_ref[...]
    for o in range(NO):
        for k in range(nw - 1):
            pow_recv(k, o).wait_recv()
        acc = pow_v[0, o]
        for w in range(1, nw):
            acc = acc + pow_v[w, o]
        scale = lax.rsqrt(acc / (C * nw) + 1e-6)
        if nb < SUB:
            scale = jnp.concatenate([scale, jnp.zeros((SUB - nb, LANES), jnp.float32)], 0)
        cols = scale.T
        for n in range(nb):
            for v in range(steps):
                wide_v[at(o, n * steps + v), :] = jnp.broadcast_to(
                    cols[v * SUB:(v + 1) * SUB, n:n + 1], (SUB, LANES))
        for s in range(o * SUB, (o + 1) * SUB):
            for j in range(0, seg, 16):
                r = pl.ds(s * pitch + j, 16)
                sc = wide_v[r, :]
                parts = [state_v[g, r, :] * sc * gain[:, g * LANES:(g + 1) * LANES] for g in range(G)]
                out_v[pl.ds(s * seg + j, 16), :] = jnp.concatenate(parts, 1).astype(jnp.bfloat16)

    for k in range(ns - 1):
        tot_send(k).wait_send()
    for o in range(NO):
        for k in range(nw - 1):
            pow_send(k, o).wait_send()


def per_device(ns, nw, leak_rate, signal_in, norm_gain):
    _, T, C = leak_rate.shape
    G = C // LANES
    seg = 64
    NS = T // seg
    NO = NS // SUB
    pitch = seg + 4
    nb = SUB * seg // LANES
    f32 = jnp.float32
    vmem = pl.BlockSpec(memory_space=pltpu.VMEM)
    hbm = pl.BlockSpec(memory_space=pl.ANY)
    out = pl.pallas_call(
        functools.partial(join_kernel, ns, nw, seg),
        out_shape=pltpu.VMEM((T, C), jnp.bfloat16),
        in_specs=[hbm, hbm, hbm],
        out_specs=vmem,
        scratch_shapes=[
            pltpu.VMEM((1, C), f32),
            pltpu.VMEM((G, NS * pitch, LANES), f32),
            pltpu.VMEM((NS * pitch, LANES), f32),
            pltpu.VMEM((T, C), f32),
            pltpu.VMEM((T, C), jnp.bfloat16),
            pltpu.VMEM((G, NS * pitch, LANES), f32),
            pltpu.VMEM((G, NS * pitch, LANES), f32),
            pltpu.VMEM((G, (seg + 1) * NS, LANES), f32),
            pltpu.VMEM((G, (seg + 1) * NS, LANES), f32),
            pltpu.VMEM((G, (seg + 1) * NS, LANES), f32),
            pltpu.VMEM((ns, 4, C), f32),
            pltpu.VMEM((nw, NO, nb, LANES), f32),
            pltpu.SemaphoreType.DMA((2, NO)),
            pltpu.SemaphoreType.DMA(()),
            pltpu.SemaphoreType.DMA((ns,)),
            pltpu.SemaphoreType.DMA((ns,)),
            pltpu.SemaphoreType.DMA((nw, NO)),
            pltpu.SemaphoreType.DMA((nw, NO)),
        ],
        compiler_params=pltpu.CompilerParams(
            collective_id=0, has_side_effects=True, vmem_limit_bytes=32 * 2 ** 20),
    )(pltpu.with_memory_space_constraint(leak_rate[0], pltpu.HBM),
      pltpu.with_memory_space_constraint(signal_in[0], pltpu.HBM),
      pltpu.with_memory_space_constraint(norm_gain[None], pltpu.HBM))
    return out[None]


def solution(mesh):
    return jax.shard_map(
        functools.partial(per_device, mesh.shape["seq"], mesh.shape["width"]),
        mesh=mesh,
        in_specs=(P(None, "seq", "width"), P(None, "seq", "width"), P("width")),
        out_specs=P(None, "seq", "width"),
        check_vma=False,
    )
```

```python
import functools

import jax
import jax.numpy as jnp
from jax import lax
from jax.experimental import pallas as pl
from jax.experimental.pallas import tpu as pltpu
from jax.sharding import PartitionSpec as P

LANES = 128
SUB = 8
MESH = pl.DeviceIdType.MESH


def join_kernel(ns, nw, seg, leak_hbm, sig_hbm, gain_hbm, out_v, gain_ref, state_v, wide_v, leak_v, sig_v, keep_v, push_v,
                local_v, pre_v, suf_v, tot_v, pow_v, in_sem, gain_sem, ts_sem, tr_sem, ps_sem, pr_sem):
    T, C = leak_v.shape
    G = C // LANES
    NS = T // seg
    NO = NS // SUB
    pitch = seg + 4
    rows = SUB * seg
    nb = rows // LANES
    total = T * ns
    me = lax.axis_index("seq")
    mw = lax.axis_index("width")

    def load(o):
        r = pl.ds(o * rows, rows)
        return (pltpu.make_async_copy(leak_hbm.at[r], leak_v.at[r], in_sem.at[0, o]),
                pltpu.make_async_copy(sig_hbm.at[r], sig_v.at[r], in_sem.at[1, o]))

    for o in range(NO):
        for c in load(o):
            c.start()

    gain_copy = pltpu.make_async_copy(gain_hbm, gain_ref, gain_sem)
    gain_copy.start()

    barrier = pltpu.get_barrier_semaphore()
    for k in range(1, ns):
        pl.semaphore_signal(barrier, inc=1, device_id={"seq": lax.rem(me + k, ns)}, device_id_type=MESH)
    for k in range(1, nw):
        pl.semaphore_signal(barrier, inc=1, device_id={"width": lax.rem(mw + k, nw)}, device_id_type=MESH)

    def at(o, i):
        return pl.ds(o * SUB * pitch + i, SUB, stride=pitch)

    def row_of(o, i):
        return pl.ds(pl.multiple_of((o * (seg + 1) + i) * SUB, SUB), SUB)

    zero = jnp.zeros((SUB, LANES), jnp.float32)
    one = jnp.ones((SUB, LANES), jnp.float32)

    def fill_octet(o):
        for c in load(o):
            c.wait()

        def fill(h, _):
            base = (o * (SUB // 2) + h)
            src = pl.multiple_of(base * 2 * seg, 2 * seg)
            dst = pl.multiple_of(base * 2 * pitch, SUB)
            for half in range(2):
                for j in range(0, seg, 16):
                    lk = leak_v[pl.ds(src + half * seg + j, 16), :]
                    kp = jnp.exp(lk * (-1.0 / total))
                    ps = sig_v[pl.ds(src + half * seg + j, 16), :].astype(jnp.float32) * (total ** -0.5)
                    for g in range(G):
                        cols = slice(g * LANES, (g + 1) * LANES)
                        for q in range(2):
                            to = pl.ds(dst + half * pitch + j + q * SUB, SUB)
                            keep_v[g, to, :] = kp[q * SUB:(q + 1) * SUB, cols]
                            push_v[g, to, :] = ps[q * SUB:(q + 1) * SUB, cols]
            return 0

        lax.fori_loop(0, SUB // 2, fill, 0)

    def segment_ends(octets):
        some = [(g, o) for g in range(G) for o in octets]

        def ends_step(i, carry):
            new = []
            for (g, o), (f, b, p) in zip(some, carry):
                k = keep_v.at[g][at(o, i), :]
                x = push_v.at[g][at(o, i), :]
                new.append((k * f + x, b + p * x, p * k))
            return tuple(new)

        return dict(zip(some, lax.fori_loop(0, seg, ends_step, tuple((zero, zero, one) for _ in some), unroll=8)))

    chains = [(g, o) for g in range(G) for o in range(NO)]
    ends = {}
    for octets in (range(NO // 2), range(NO // 2, NO)):
        for o in octets:
            fill_octet(o)
        ends.update(segment_ends(octets))

    def gathered(which):
        return jnp.concatenate(
            [jnp.concatenate([ends[g, o][which] for o in range(NO)], 0) for g in range(G)], 1)

    f_end, b_end, p_end = gathered(0), gathered(1), gathered(2)
    row = lax.broadcasted_iota(jnp.int32, (NS, C), 0)

    def shifted(x, d, fill):
        if d > 0:
            return jnp.where(row >= d, pltpu.roll(x, d, 0), fill)
        return jnp.where(row < NS + d, pltpu.roll(x, NS + d, 0), fill)

    pf, ff = p_end, f_end
    pb, bb = p_end, b_end
    d = 1
    while d < NS:
        ff = ff + pf * shifted(ff, d, 0.0)
        pf = pf * shifted(pf, d, 1.0)
        bb = bb + pb * shifted(bb, -d, 0.0)
        pb = pb * shifted(pb, -d, 1.0)
        d *= 2
    tot_v[me] = jnp.concatenate(
        [pf[NS - 1:NS], ff[NS - 1:NS], bb[0:1], jnp.zeros((1, C), jnp.float32)], 0)

    pl.semaphore_wait(barrier, ns + nw - 2)

    def other(k, own):
        return k + jnp.where(k >= own, 1, 0)

    def tot_send(k):
        return pltpu.make_async_remote_copy(
            src_ref=tot_v.at[me], dst_ref=tot_v.at[me], send_sem=ts_sem, recv_sem=tr_sem,
            device_id={"seq": other(k, me)}, device_id_type=MESH)

    def tot_all():
        every = tot_v.at[pl.ds(0, ns - 1)]
        return pltpu.make_async_remote_copy(
            src_ref=every, dst_ref=every, send_sem=ts_sem, recv_sem=tr_sem,
            device_id={"seq": other(0, me)}, device_id_type=MESH)

    for k in range(ns - 1):
        tot_send(k).start()

    def ahead(i, carry):
        new = []
        for (g, o), (f, p) in zip(chains, carry):
            k = keep_v.at[g][at(o, i), :]
            x = push_v.at[g][at(o, i), :]
            f = k * f + x
            p = p * k
            local_v[g, row_of(o, i), :] = f
            pre_v[g, row_of(o, i), :] = p
            new.append((f, p))
        return tuple(new)

    lax.fori_loop(0, seg, ahead, tuple((zero, one) for _ in chains), unroll=4)

    def back(n, carry):
        i = seg - 1 - n
        new = []
        for (g, o), (b, q) in zip(chains, carry):
            k = keep_v.at[g][at(o, i), :]
            x = push_v.at[g][at(o, i), :]
            b = k * b + x
            q = k * q
            r = row_of(o, i)
            local_v[g, r, :] = local_v[g, r, :] + b
            suf_v[g, r, :] = q
            new.append((b, q))
        return tuple(new)

    lax.fori_loop(0, seg, back, tuple((zero, one) for _ in chains), unroll=4)

    tot_all().wait_recv()
    f_in = jnp.zeros((1, C), jnp.float32)
    b_in = jnp.zeros((1, C), jnp.float32)
    for j in range(ns):
        t = tot_v[j]
        f_in = jnp.where(j < me, t[0:1] * f_in + t[1:2], f_in)
        t = tot_v[ns - 1 - j]
        b_in = jnp.where(ns - 1 - j > me, t[0:1] * b_in + t[2:3], b_in)
    f_in = shifted(ff, 1, 0.0) + shifted(pf, 1, 1.0) * f_in
    b_in = shifted(bb, -1, 0.0) + shifted(pb, -1, 1.0) * b_in

    ones = jnp.ones((SUB, LANES), jnp.bfloat16)
    nt = (((1,), (1,)), ((), ()))

    def flipped(w):
        return w + 1 - 2 * lax.rem(w, 2)

    def pow_send(k, o):
        return pltpu.make_async_remote_copy(
            src_ref=pow_v.at[mw, o], dst_ref=pow_v.at[mw, o], send_sem=ps_sem.at[o], recv_sem=pr_sem.at[o],
            device_id={"width": flipped(other(k, flipped(mw)))}, device_id_type=MESH)

    def pow_all(o):
        every = pow_v.at[pl.ds(0, nw - 1), o]
        return pltpu.make_async_remote_copy(
            src_ref=every, dst_ref=every, send_sem=ps_sem.at[o], recv_sem=pr_sem.at[o],
            device_id={"width": other(0, mw)}, device_id_type=MESH)

    steps = LANES // SUB
    pending = []

    def store_power(b, res):
        o, n = divmod(b, nb)
        pow_v[mw, o, pl.ds(n, 1), :] = res[0:1]
        if n == nb - 1:
            for k in range(nw - 1):
                pow_send(k, o).start()

    for b in range(NO * nb):
        o, n = divmod(b, nb)
        sq = []
        for i in range(n * steps, (n + 1) * steps):
            x = None
            r = pl.ds((o * (seg + 1) + i) * SUB, SUB)
            for g in range(G):
                c = slice(g * LANES, (g + 1) * LANES)
                st = (local_v[g, r, :] + pre_v[g, r, :] * f_in[o * SUB:(o + 1) * SUB, c]
                      + suf_v[g, r, :] * b_in[o * SUB:(o + 1) * SUB, c])
                state_v.at[g][at(o, i), :] = st
                x = st * st if x is None else x + st * st
            sq.append(x)
        x = jnp.concatenate(sq, 0)
        hi = x.astype(jnp.bfloat16)
        lo = (x - hi.astype(jnp.float32)).astype(jnp.bfloat16)
        pending.append((b, lax.dot_general(ones, hi, nt, preferred_element_type=jnp.float32)
                        + lax.dot_general(ones, lo, nt, preferred_element_type=jnp.float32)))
        if len(pending) > 2:
            store_power(*pending.pop(0))
    for p in pending:
        store_power(*p)

    gain_copy.wait()
    gain = gain_ref[...]
    for o in range(NO):
        pow_all(o).wait_recv()
        acc = pow_v[0, o]
        for w in range(1, nw):
            acc = acc + pow_v[w, o]
        scale = lax.rsqrt(acc / (C * nw) + 1e-6)
        if nb < SUB:
            scale = jnp.concatenate([scale, jnp.zeros((SUB - nb, LANES), jnp.float32)], 0)
        cols = scale.T
        for n in range(nb):
            for v in range(steps):
                wide_v[at(o, n * steps + v), :] = jnp.broadcast_to(
                    cols[v * SUB:(v + 1) * SUB, n:n + 1], (SUB, LANES))
        for s in range(o * SUB, (o + 1) * SUB):
            for j in range(0, seg, 16):
                r = pl.ds(s * pitch + j, 16)
                sc = wide_v[r, :]
                parts = [state_v[g, r, :] * sc * gain[:, g * LANES:(g + 1) * LANES] for g in range(G)]
                out_v[pl.ds(s * seg + j, 16), :] = jnp.concatenate(parts, 1).astype(jnp.bfloat16)

    tot_all().wait_send()
    for o in range(NO):
        pow_all(o).wait_send()


def per_device(ns, nw, leak_rate, signal_in, norm_gain):
    _, T, C = leak_rate.shape
    G = C // LANES
    seg = 64
    NS = T // seg
    NO = NS // SUB
    pitch = seg + 4
    nb = SUB * seg // LANES
    f32 = jnp.float32
    vmem = pl.BlockSpec(memory_space=pltpu.VMEM)
    hbm = pl.BlockSpec(memory_space=pl.ANY)
    out = pl.pallas_call(
        functools.partial(join_kernel, ns, nw, seg),
        out_shape=pltpu.VMEM((T, C), jnp.bfloat16),
        in_specs=[hbm, hbm, hbm],
        out_specs=vmem,
        scratch_shapes=[
            pltpu.VMEM((1, C), f32),
            pltpu.VMEM((G, NS * pitch, LANES), f32),
            pltpu.VMEM((NS * pitch, LANES), f32),
            pltpu.VMEM((T, C), f32),
            pltpu.VMEM((T, C), jnp.bfloat16),
            pltpu.VMEM((G, NS * pitch, LANES), f32),
            pltpu.VMEM((G, NS * pitch, LANES), f32),
            pltpu.VMEM((G, (seg + 1) * NS, LANES), f32),
            pltpu.VMEM((G, (seg + 1) * NS, LANES), f32),
            pltpu.VMEM((G, (seg + 1) * NS, LANES), f32),
            pltpu.VMEM((ns, 4, C), f32),
            pltpu.VMEM((nw, NO, nb, LANES), f32),
            pltpu.SemaphoreType.DMA((2, NO)),
            pltpu.SemaphoreType.DMA(()),
            pltpu.SemaphoreType.DMA(()),
            pltpu.SemaphoreType.DMA(()),
            pltpu.SemaphoreType.DMA((NO,)),
            pltpu.SemaphoreType.DMA((NO,)),
        ],
        compiler_params=pltpu.CompilerParams(
            collective_id=0, has_side_effects=True, vmem_limit_bytes=32 * 2 ** 20),
    )(pltpu.with_memory_space_constraint(leak_rate[0], pltpu.HBM),
      pltpu.with_memory_space_constraint(signal_in[0], pltpu.HBM),
      pltpu.with_memory_space_constraint(norm_gain[None], pltpu.HBM))
    return out[None]


def solution(mesh):
    return jax.shard_map(
        functools.partial(per_device, mesh.shape["seq"], mesh.shape["width"]),
        mesh=mesh,
        in_specs=(P(None, "seq", "width"), P(None, "seq", "width"), P("width")),
        out_specs=P(None, "seq", "width"),
        check_vma=False,
    )
```

```python
import functools

import jax
import jax.numpy as jnp
from jax import lax
from jax.experimental import pallas as pl
from jax.experimental.pallas import tpu as pltpu
from jax.sharding import PartitionSpec as P

LANES = 128
SUB = 8
MESH = pl.DeviceIdType.MESH


def join_kernel(ns, nw, seg, leak_hbm, sig_hbm, gain_hbm, out_v, gain_ref, state_v, wide_v, leak_v, sig_v, keep_v, push_v,
                local_v, pre_v, suf_v, tot_v, pow_v, in_sem, gain_sem, ts_sem, tr_sem, ps_sem, pr_sem):
    T, C = leak_v.shape
    G = C // LANES
    NS = T // seg
    NO = NS // SUB
    pitch = seg + 4
    rows = SUB * seg
    nb = rows // LANES
    total = T * ns
    me = lax.axis_index("seq")
    mw = lax.axis_index("width")

    def load(o):
        r = pl.ds(o * rows, rows)
        return (pltpu.make_async_copy(leak_hbm.at[r], leak_v.at[r], in_sem.at[0, o]),
                pltpu.make_async_copy(sig_hbm.at[r], sig_v.at[r], in_sem.at[1, o]))

    for o in range(NO):
        for c in load(o):
            c.start()

    gain_copy = pltpu.make_async_copy(gain_hbm, gain_ref, gain_sem)
    gain_copy.start()

    barrier = pltpu.get_barrier_semaphore()
    for k in sorted(range(1, nw), key=lambda k: abs(min(k, nw - k) - 3 * nw // 8)):
        pl.semaphore_signal(barrier, inc=1, device_id={"width": lax.rem(mw + k, nw)}, device_id_type=MESH)
    for k in sorted(range(1, ns), key=lambda k: abs(min(k, ns - k) - 4)):
        pl.semaphore_signal(barrier, inc=1, device_id={"seq": lax.rem(me + k, ns)}, device_id_type=MESH)

    def at(o, i):
        return pl.ds(o * SUB * pitch + i, SUB, stride=pitch)

    def row_of(o, i):
        return pl.ds(pl.multiple_of((o * (seg + 1) + i) * SUB, SUB), SUB)

    zero = jnp.zeros((SUB, LANES), jnp.float32)
    one = jnp.ones((SUB, LANES), jnp.float32)

    def fill_octet(o):
        for c in load(o):
            c.wait()

        def fill(h, _):
            base = (o * (SUB // 2) + h)
            src = pl.multiple_of(base * 2 * seg, 2 * seg)
            dst = pl.multiple_of(base * 2 * pitch, SUB)
            for half in range(2):
                for j in range(0, seg, 16):
                    lk = leak_v[pl.ds(src + half * seg + j, 16), :]
                    kp = jnp.exp(lk * (-1.0 / total))
                    ps = sig_v[pl.ds(src + half * seg + j, 16), :].astype(jnp.float32) * (total ** -0.5)
                    for g in range(G):
                        cols = slice(g * LANES, (g + 1) * LANES)
                        for q in range(2):
                            to = pl.ds(dst + half * pitch + j + q * SUB, SUB)
                            keep_v[g, to, :] = kp[q * SUB:(q + 1) * SUB, cols]
                            push_v[g, to, :] = ps[q * SUB:(q + 1) * SUB, cols]
            return 0

        lax.fori_loop(0, SUB // 2, fill, 0)

    def segment_ends(octets):
        some = [(g, o) for g in range(G) for o in octets]

        def ends_step(i, carry):
            new = []
            for (g, o), (f, b, p) in zip(some, carry):
                k = keep_v.at[g][at(o, i), :]
                x = push_v.at[g][at(o, i), :]
                new.append((k * f + x, b + p * x, p * k))
            return tuple(new)

        return dict(zip(some, lax.fori_loop(0, seg, ends_step, tuple((zero, zero, one) for _ in some), unroll=8)))

    chains = [(g, o) for g in range(G) for o in range(NO)]
    ends = {}
    for octets in (range(NO // 2), range(NO // 2, NO)):
        for o in octets:
            fill_octet(o)
        ends.update(segment_ends(octets))

    def gathered(which):
        return jnp.concatenate(
            [jnp.concatenate([ends[g, o][which] for o in range(NO)], 0) for g in range(G)], 1)

    f_end, b_end, p_end = gathered(0), gathered(1), gathered(2)
    row = lax.broadcasted_iota(jnp.int32, (NS, C), 0)

    def shifted(x, d, fill):
        if d > 0:
            return jnp.where(row >= d, pltpu.roll(x, d, 0), fill)
        return jnp.where(row < NS + d, pltpu.roll(x, NS + d, 0), fill)

    pf, ff = p_end, f_end
    pb, bb = p_end, b_end
    d = 1
    while d < NS:
        ff = ff + pf * shifted(ff, d, 0.0)
        pf = pf * shifted(pf, d, 1.0)
        bb = bb + pb * shifted(bb, -d, 0.0)
        pb = pb * shifted(pb, -d, 1.0)
        d *= 2
    tot_v[me] = jnp.concatenate(
        [pf[NS - 1:NS], ff[NS - 1:NS], bb[0:1], jnp.zeros((1, C), jnp.float32)], 0)

    pl.semaphore_wait(barrier, ns + nw - 2)

    def other(k, own):
        return k + jnp.where(k >= own, 1, 0)

    def tot_send(k):
        return pltpu.make_async_remote_copy(
            src_ref=tot_v.at[me], dst_ref=tot_v.at[me], send_sem=ts_sem, recv_sem=tr_sem,
            device_id={"seq": other(k, me)}, device_id_type=MESH)

    def tot_all():
        every = tot_v.at[pl.ds(0, ns - 1)]
        return pltpu.make_async_remote_copy(
            src_ref=every, dst_ref=every, send_sem=ts_sem, recv_sem=tr_sem,
            device_id={"seq": other(0, me)}, device_id_type=MESH)

    for k in range(ns - 1):
        tot_send(k).start()

    def ahead(i, carry):
        new = []
        for (g, o), (f, p) in zip(chains, carry):
            k = keep_v.at[g][at(o, i), :]
            x = push_v.at[g][at(o, i), :]
            f = k * f + x
            p = p * k
            local_v[g, row_of(o, i), :] = f
            pre_v[g, row_of(o, i), :] = p
            new.append((f, p))
        return tuple(new)

    lax.fori_loop(0, seg, ahead, tuple((zero, one) for _ in chains), unroll=4)

    def back(n, carry):
        i = seg - 1 - n
        new = []
        for (g, o), (b, q) in zip(chains, carry):
            k = keep_v.at[g][at(o, i), :]
            x = push_v.at[g][at(o, i), :]
            b = k * b + x
            q = k * q
            r = row_of(o, i)
            local_v[g, r, :] = local_v[g, r, :] + b
            suf_v[g, r, :] = q
            new.append((b, q))
        return tuple(new)

    lax.fori_loop(0, seg, back, tuple((zero, one) for _ in chains), unroll=4)

    tot_all().wait_recv()
    f_in = jnp.zeros((1, C), jnp.float32)
    b_in = jnp.zeros((1, C), jnp.float32)
    for j in range(ns):
        t = tot_v[j]
        f_in = jnp.where(j < me, t[0:1] * f_in + t[1:2], f_in)
        t = tot_v[ns - 1 - j]
        b_in = jnp.where(ns - 1 - j > me, t[0:1] * b_in + t[2:3], b_in)
    f_in = shifted(ff, 1, 0.0) + shifted(pf, 1, 1.0) * f_in
    b_in = shifted(bb, -1, 0.0) + shifted(pb, -1, 1.0) * b_in

    ones = jnp.ones((SUB, LANES), jnp.bfloat16)
    nt = (((1,), (1,)), ((), ()))

    def pow_now(w, o):
        return pltpu.make_async_remote_copy(
            src_ref=pow_v.at[mw, o], dst_ref=pow_v.at[mw, o], send_sem=ps_sem, recv_sem=pr_sem.at[o],
            device_id={"width": w}, device_id_type=MESH)

    def pow_bulk(w):
        return pltpu.make_async_remote_copy(
            src_ref=pow_v.at[mw], dst_ref=pow_v.at[mw], send_sem=ps_sem, recv_sem=pr_sem.at[0],
            device_id={"width": w}, device_id_type=MESH)

    def pow_chunk(o):
        every = pow_v.at[pl.ds(0, nw - 1), o]
        return pltpu.make_async_remote_copy(
            src_ref=every, dst_ref=every, send_sem=ps_sem, recv_sem=pr_sem.at[o],
            device_id={"width": other(0, mw)}, device_id_type=MESH)

    def pow_all():
        every = pow_v.at[pl.ds(0, nw - 1)]
        return pltpu.make_async_remote_copy(
            src_ref=every, dst_ref=every, send_sem=ps_sem, recv_sem=pr_sem.at[0],
            device_id={"width": other(0, mw)}, device_id_type=MESH)

    steps = LANES // SUB
    pending = []

    def store_power(b, res):
        o, n = divmod(b, nb)
        pow_v[mw, o, pl.ds(n, 1), :] = res[0:1]
        if n == nb - 1:
            for w in (1, 0):
                @pl.when(mw != w)
                def _():
                    pow_now(w, o).start()

    for b in range(NO * nb):
        o, n = divmod(b, nb)
        sq = []
        for i in range(n * steps, (n + 1) * steps):
            x = None
            r = pl.ds((o * (seg + 1) + i) * SUB, SUB)
            for g in range(G):
                c = slice(g * LANES, (g + 1) * LANES)
                st = (local_v[g, r, :] + pre_v[g, r, :] * f_in[o * SUB:(o + 1) * SUB, c]
                      + suf_v[g, r, :] * b_in[o * SUB:(o + 1) * SUB, c])
                state_v.at[g][at(o, i), :] = st
                x = st * st if x is None else x + st * st
            sq.append(x)
        x = jnp.concatenate(sq, 0)
        hi = x.astype(jnp.bfloat16)
        lo = (x - hi.astype(jnp.float32)).astype(jnp.bfloat16)
        pending.append((b, lax.dot_general(ones, hi, nt, preferred_element_type=jnp.float32)
                        + lax.dot_general(ones, lo, nt, preferred_element_type=jnp.float32)))
        if len(pending) > 2:
            store_power(*pending.pop(0))
    for p in pending:
        store_power(*p)
    @pl.when(mw < 2)
    def _():
        pow_bulk(2).start()
    for k in range(nw - 3):
        pow_bulk(k + 2 + jnp.where(k + 2 >= mw, 1, 0)).start()

    gain_copy.wait()
    gain = gain_ref[...]
    for o in range(NO):
        @pl.when(mw < 2)
        def _():
            pow_chunk(o).wait_recv()
        if o == 0:
            @pl.when(mw >= 2)
            def _():
                pow_all().wait_recv()
        acc = pow_v[0, o]
        for w in range(1, nw):
            acc = acc + pow_v[w, o]
        scale = lax.rsqrt(acc / (C * nw) + 1e-6)
        if nb < SUB:
            scale = jnp.concatenate([scale, jnp.zeros((SUB - nb, LANES), jnp.float32)], 0)
        cols = scale.T
        for n in range(nb):
            for v in range(steps):
                wide_v[at(o, n * steps + v), :] = jnp.broadcast_to(
                    cols[v * SUB:(v + 1) * SUB, n:n + 1], (SUB, LANES))
        for s in range(o * SUB, (o + 1) * SUB):
            for j in range(0, seg, 16):
                r = pl.ds(s * pitch + j, 16)
                sc = wide_v[r, :]
                parts = [state_v[g, r, :] * sc * gain[:, g * LANES:(g + 1) * LANES] for g in range(G)]
                out_v[pl.ds(s * seg + j, 16), :] = jnp.concatenate(parts, 1).astype(jnp.bfloat16)

    tot_all().wait_send()
    pow_all().wait_send()


def per_device(ns, nw, leak_rate, signal_in, norm_gain):
    _, T, C = leak_rate.shape
    G = C // LANES
    seg = 64
    NS = T // seg
    NO = NS // SUB
    pitch = seg + 4
    nb = SUB * seg // LANES
    f32 = jnp.float32
    vmem = pl.BlockSpec(memory_space=pltpu.VMEM)
    hbm = pl.BlockSpec(memory_space=pl.ANY)
    out = pl.pallas_call(
        functools.partial(join_kernel, ns, nw, seg),
        out_shape=pltpu.VMEM((T, C), jnp.bfloat16),
        in_specs=[hbm, hbm, hbm],
        out_specs=vmem,
        scratch_shapes=[
            pltpu.VMEM((1, C), f32),
            pltpu.VMEM((G, NS * pitch, LANES), f32),
            pltpu.VMEM((NS * pitch, LANES), f32),
            pltpu.VMEM((T, C), f32),
            pltpu.VMEM((T, C), jnp.bfloat16),
            pltpu.VMEM((G, NS * pitch, LANES), f32),
            pltpu.VMEM((G, NS * pitch, LANES), f32),
            pltpu.VMEM((G, (seg + 1) * NS, LANES), f32),
            pltpu.VMEM((G, (seg + 1) * NS, LANES), f32),
            pltpu.VMEM((G, (seg + 1) * NS, LANES), f32),
            pltpu.VMEM((ns, 4, C), f32),
            pltpu.VMEM((nw, NO, nb, LANES), f32),
            pltpu.SemaphoreType.DMA((2, NO)),
            pltpu.SemaphoreType.DMA(()),
            pltpu.SemaphoreType.DMA(()),
            pltpu.SemaphoreType.DMA(()),
            pltpu.SemaphoreType.DMA(()),
            pltpu.SemaphoreType.DMA((NO,)),
        ],
        compiler_params=pltpu.CompilerParams(
            collective_id=0, has_side_effects=True, vmem_limit_bytes=32 * 2 ** 20),
    )(pltpu.with_memory_space_constraint(leak_rate[0], pltpu.HBM),
      pltpu.with_memory_space_constraint(signal_in[0], pltpu.HBM),
      pltpu.with_memory_space_constraint(norm_gain[None], pltpu.HBM))
    return out[None]


def solution(mesh):
    return jax.shard_map(
        functools.partial(per_device, mesh.shape["seq"], mesh.shape["width"]),
        mesh=mesh,
        in_specs=(P(None, "seq", "width"), P(None, "seq", "width"), P("width")),
        out_specs=P(None, "seq", "width"),
        check_vma=False,
    )
```

```python
import functools

import jax
import jax.numpy as jnp
from jax import lax
from jax.experimental import pallas as pl
from jax.experimental.pallas import tpu as pltpu
from jax.sharding import PartitionSpec as P

LANES = 128
SUB = 8
MESH = pl.DeviceIdType.MESH


def join_kernel(ns, nw, seg, leak_hbm, sig_hbm, gain_hbm, out_v, gain_ref, state_v, leak_v, sig_v, keep_v, push_v,
                pre_v, suf_v, tot_v, pow_v, in_sem, gain_sem, ts_sem, tr_sem, ps_sem, pr_sem):
    T, C = leak_v.shape
    NS = T // seg
    NO = NS // SUB
    NB = T // LANES
    pitch = seg + 4
    rows = SUB * seg
    total = T * ns
    me = lax.axis_index("seq")
    mw = lax.axis_index("width")

    def load(o):
        r = pl.ds(o * rows, rows)
        return (pltpu.make_async_copy(leak_hbm.at[r], leak_v.at[r], in_sem.at[0, o]),
                pltpu.make_async_copy(sig_hbm.at[r], sig_v.at[r], in_sem.at[1, o]))

    for o in range(NO):
        for c in load(o):
            c.start()

    gain_copy = pltpu.make_async_copy(gain_hbm, gain_ref, gain_sem)
    gain_copy.start()

    barrier = pltpu.get_barrier_semaphore()
    for k in sorted(range(1, nw), key=lambda k: abs(min(k, nw - k) - 3 * nw // 8)):
        pl.semaphore_signal(barrier, inc=1, device_id={"width": lax.rem(mw + k, nw)}, device_id_type=MESH)
    for k in sorted(range(1, ns), key=lambda k: abs(min(k, ns - k) - 4)):
        pl.semaphore_signal(barrier, inc=1, device_id={"seq": lax.rem(me + k, ns)}, device_id_type=MESH)

    def at(o, i):
        return pl.ds(o * SUB * pitch + i, SUB, stride=pitch)

    zero = jnp.zeros((SUB, LANES), jnp.float32)
    one = jnp.ones((SUB, LANES), jnp.float32)

    def fill_octet(o):
        for c in load(o):
            c.wait()

        def fill(h, _):
            base = (o * (SUB // 2) + h)
            src = pl.multiple_of(base * 2 * seg, 2 * seg)
            dst = pl.multiple_of(base * 2 * pitch, SUB)
            for half in range(2):
                for j in range(0, seg, 16):
                    lk = leak_v[pl.ds(src + half * seg + j, 16), :]
                    kp = jnp.exp(lk * (-1.0 / total))
                    ps = sig_v[pl.ds(src + half * seg + j, 16), :].astype(jnp.float32) * (total ** -0.5)
                    to = pl.ds(dst + half * pitch + j, 2 * SUB)
                    keep_v[to, :] = kp
                    push_v[to, :] = ps
            return 0

        lax.fori_loop(0, SUB // 2, fill, 0)

    def segment_ends(octets):
        def ends_step(i, carry):
            new = []
            for o, (f, b, p) in zip(octets, carry):
                k = keep_v[at(o, i), :]
                x = push_v[at(o, i), :]
                new.append((k * f + x, b + p * x, p * k))
            return tuple(new)

        return lax.fori_loop(0, seg, ends_step, tuple((zero, zero, one) for _ in octets), unroll=8)

    ends = []
    for octets in (range(NO // 2), range(NO // 2, NO)):
        for o in octets:
            fill_octet(o)
        ends.extend(segment_ends(octets))

    def gathered(which):
        return jnp.concatenate([e[which] for e in ends], 0)

    f_end, b_end, p_end = gathered(0), gathered(1), gathered(2)
    row = lax.broadcasted_iota(jnp.int32, (NS, C), 0)

    def shifted(x, d, fill):
        if d > 0:
            return jnp.where(row >= d, pltpu.roll(x, d, 0), fill)
        return jnp.where(row < NS + d, pltpu.roll(x, NS + d, 0), fill)

    pf, ff = p_end, f_end
    pb, bb = p_end, b_end
    d = 1
    while d < NS:
        ff = ff + pf * shifted(ff, d, 0.0)
        pf = pf * shifted(pf, d, 1.0)
        bb = bb + pb * shifted(bb, -d, 0.0)
        pb = pb * shifted(pb, -d, 1.0)
        d *= 2
    tot_v[me] = jnp.concatenate(
        [pf[NS - 1:NS], ff[NS - 1:NS], bb[0:1], jnp.zeros((1, C), jnp.float32)], 0)

    pl.semaphore_wait(barrier, ns + nw - 2)

    def other(k, own):
        return k + jnp.where(k >= own, 1, 0)

    def tot_send(k):
        return pltpu.make_async_remote_copy(
            src_ref=tot_v.at[me], dst_ref=tot_v.at[me], send_sem=ts_sem, recv_sem=tr_sem,
            device_id={"seq": other(k, me)}, device_id_type=MESH)

    def tot_all():
        every = tot_v.at[pl.ds(0, ns - 1)]
        return pltpu.make_async_remote_copy(
            src_ref=every, dst_ref=every, send_sem=ts_sem, recv_sem=tr_sem,
            device_id={"seq": other(0, me)}, device_id_type=MESH)

    for k in range(ns - 1):
        tot_send(k).start()

    def octets_of(x):
        return [x[o * SUB:(o + 1) * SUB] for o in range(NO)]

    f_from, p_from = octets_of(shifted(ff, 1, 0.0)), octets_of(shifted(pf, 1, 1.0))
    b_from, q_from = octets_of(shifted(bb, -1, 0.0)), octets_of(shifted(pb, -1, 1.0))

    def ahead(i, carry):
        new = []
        for o, (f, p) in enumerate(carry):
            r = at(o, i)
            k = keep_v[r, :]
            f = k * f + push_v[r, :]
            p = p * k
            state_v[r, :] = f
            pre_v[r, :] = p
            new.append((f, p))
        return tuple(new)

    lax.fori_loop(0, seg, ahead, tuple(zip(f_from, p_from)), unroll=4)

    def back(n, carry):
        i = seg - 1 - n
        new = []
        for o, (b, q) in enumerate(carry):
            r = at(o, i)
            k = keep_v[r, :]
            b = k * b + push_v[r, :]
            q = k * q
            state_v[r, :] = state_v[r, :] + b
            suf_v[r, :] = q
            new.append((b, q))
        return tuple(new)

    lax.fori_loop(0, seg, back, tuple(zip(b_from, q_from)), unroll=4)

    tot_all().wait_recv()
    def folded(which, mask, later_first):
        p = jnp.where(mask, tot_v[:, 0, :], 1.0)
        x = jnp.where(mask, tot_v[:, which, :], 0.0)
        n = ns
        while n > 1:
            d = ns // n
            pl_, xl = pltpu.roll(p, ns - d, 0), pltpu.roll(x, ns - d, 0)
            x = x + p * xl if later_first else pl_ * x + xl
            p = p * pl_
            n //= 2
        return jnp.broadcast_to(x[0:1], (SUB, C))

    who = lax.broadcasted_iota(jnp.int32, (ns, C), 0)
    f_in = folded(1, who < me, False)
    b_in = folded(2, who > me, True)

    ones = jnp.ones((SUB, 2 * LANES), jnp.bfloat16)
    nt = (((1,), (1,)), ((), ()))

    def pow_now(w, h):
        part = pow_v.at[mw, pl.ds(h * SUB, SUB)]
        return pltpu.make_async_remote_copy(
            src_ref=part, dst_ref=part, send_sem=ps_sem, recv_sem=pr_sem, device_id={"width": w}, device_id_type=MESH)

    def pow_bulk(w):
        return pltpu.make_async_remote_copy(
            src_ref=pow_v.at[mw], dst_ref=pow_v.at[mw], send_sem=ps_sem, recv_sem=pr_sem,
            device_id={"width": w}, device_id_type=MESH)

    def pow_all():
        every = pow_v.at[pl.ds(0, nw - 1)]
        return pltpu.make_async_remote_copy(
            src_ref=every, dst_ref=every, send_sem=ps_sem, recv_sem=pr_sem,
            device_id={"width": other(0, mw)}, device_id_type=MESH)

    def rows_of(b):
        return [pl.ds((b * LANES + j) // seg * pitch + (b * LANES + j) % seg, 2 * SUB) for j in range(0, LANES, 2 * SUB)]

    pending = []

    def store_power(b, res):
        pow_v[mw, pl.ds(b, 1), :] = res[0:1, :LANES]
        pow_v[mw, pl.ds(b + 1, 1), :] = res[0:1, LANES:]
        if (b + 2) % SUB == 0:
            for w in (1, 0):
                @pl.when(mw != w)
                def _():
                    pow_now(w, b // SUB).start()

    f16, b16 = jnp.concatenate([f_in] * 2, 0), jnp.concatenate([b_in] * 2, 0)
    for b in range(0, NB, 2):
        hi, lo = [], []
        for r in rows_of(b) + rows_of(b + 1):
            st = state_v[r, :] + pre_v[r, :] * f16 + suf_v[r, :] * b16
            state_v[r, :] = st
            x = st * st
            h = x.astype(jnp.bfloat16)
            hi.append(h)
            lo.append((x - h.astype(jnp.float32)).astype(jnp.bfloat16))
        both = jnp.concatenate([jnp.concatenate(hi, 0), jnp.concatenate(lo, 0)], 1)
        pending.append((b, lax.dot_general(ones, both, nt, preferred_element_type=jnp.float32)))
        if len(pending) > 1:
            store_power(*pending.pop(0))
    for p in pending:
        store_power(*p)

    @pl.when(mw < 2)
    def _():
        pow_bulk(2).start()
    for k in range(nw - 3):
        pow_bulk(k + 2 + jnp.where(k + 2 >= mw, 1, 0)).start()

    gain_copy.wait()
    gain = jnp.broadcast_to(gain_ref[...], (2 * SUB, C))

    def times_gain(s, _):
        for j in range(0, seg, 2 * SUB):
            r = pl.ds(s * pitch + j, 2 * SUB)
            state_v[r, :] = state_v[r, :] * gain
        return 0

    lax.fori_loop(0, NS, times_gain, 0)

    pow_all().wait_recv()
    acc = pow_v[0]
    for w in range(1, nw):
        acc = acc + pow_v[w]
    scale = lax.rsqrt(acc / (C * nw) + 1e-6)
    for h in range(NB // SUB):
        cols = scale[h * SUB:(h + 1) * SUB].T
        for n in range(SUB):
            b = h * SUB + n
            wide = jnp.broadcast_to(cols[:, n:n + 1], (LANES, LANES))
            for q, r in enumerate(rows_of(b)):
                out_v[pl.ds(b * LANES + q * 2 * SUB, 2 * SUB), :] = (
                    state_v[r, :] * wide[q * 2 * SUB:(q + 1) * 2 * SUB]).astype(jnp.bfloat16)

    tot_all().wait_send()
    pow_all().wait_send()


def per_device(ns, nw, leak_rate, signal_in, norm_gain):
    _, T, C = leak_rate.shape
    seg = 64
    NS = T // seg
    NO = NS // SUB
    pitch = seg + 4
    f32 = jnp.float32
    vmem = pl.BlockSpec(memory_space=pltpu.VMEM)
    hbm = pl.BlockSpec(memory_space=pl.ANY)
    out = pl.pallas_call(
        functools.partial(join_kernel, ns, nw, seg),
        out_shape=pltpu.VMEM((T, C), jnp.bfloat16),
        in_specs=[hbm, hbm, hbm],
        out_specs=vmem,
        scratch_shapes=[
            pltpu.VMEM((1, C), f32),
            pltpu.VMEM((NS * pitch, C), f32),
            pltpu.VMEM((T, C), f32),
            pltpu.VMEM((T, C), jnp.bfloat16),
            pltpu.VMEM((NS * pitch, C), f32),
            pltpu.VMEM((NS * pitch, C), f32),
            pltpu.VMEM((NS * pitch, C), f32),
            pltpu.VMEM((NS * pitch, C), f32),
            pltpu.VMEM((ns, 4, C), f32),
            pltpu.VMEM((nw, T // LANES, LANES), f32),
            pltpu.SemaphoreType.DMA((2, NO)),
            pltpu.SemaphoreType.DMA(()),
            pltpu.SemaphoreType.DMA(()),
            pltpu.SemaphoreType.DMA(()),
            pltpu.SemaphoreType.DMA(()),
            pltpu.SemaphoreType.DMA(()),
        ],
        compiler_params=pltpu.CompilerParams(
            collective_id=0, has_side_effects=True, vmem_limit_bytes=32 * 2 ** 20),
    )(pltpu.with_memory_space_constraint(leak_rate[0], pltpu.HBM),
      pltpu.with_memory_space_constraint(signal_in[0], pltpu.HBM),
      pltpu.with_memory_space_constraint(norm_gain[None], pltpu.HBM))
    return out[None]


def solution(mesh):
    return jax.shard_map(
        functools.partial(per_device, mesh.shape["seq"], mesh.shape["width"]),
        mesh=mesh,
        in_specs=(P(None, "seq", "width"), P(None, "seq", "width"), P("width")),
        out_specs=P(None, "seq", "width"),
        check_vma=False,
    )
```

```python
import functools
import math

import jax
import jax.numpy as jnp
from jax import lax
from jax.experimental import pallas as pl
from jax.experimental.pallas import tpu as pltpu
from jax.sharding import PartitionSpec as P

LANES = 128
SUB = 8
MESH = pl.DeviceIdType.MESH


def join_kernel(ns, nw, seg, leak_hbm, sig_hbm, gain_hbm, out_v, gain_ref, state_v, leak_v, sig_v, push_v,
                pre_v, suf_v, tot_v, pow_v, in_sem, tr_sem, ps_sem, pr_sem):
    T, C = sig_v.shape
    NS = T // seg
    NO = NS // SUB
    NB = T // LANES
    pitch = seg + 4
    rows = SUB * seg
    total = T * ns
    me = lax.axis_index("seq")
    mw = lax.axis_index("width")

    def load(o):
        r = pl.ds(o * rows, rows)
        yield pltpu.make_async_copy(sig_hbm.at[r], sig_v.at[r], in_sem.at[o])
        for n in range(o * SUB, (o + 1) * SUB):
            yield pltpu.make_async_copy(
                leak_hbm.at[pl.ds(n * seg, seg)], leak_v.at[pl.ds(n * pitch, seg)], in_sem.at[o])

    def loaded(o):
        every = pl.ds(0, rows + rows // 2)
        return pltpu.make_async_copy(leak_hbm.at[every], leak_v.at[every], in_sem.at[o])

    for o in range(NO):
        for c in load(o):
            c.start()

    gain_copy = pltpu.make_async_copy(gain_hbm, gain_ref, in_sem.at[NO])
    gain_copy.start()

    barrier = pltpu.get_barrier_semaphore()
    for k in sorted(range(1, nw), key=lambda k: abs(min(k, nw - k) - 3 * nw // 8)):
        pl.semaphore_signal(barrier, inc=1, device_id={"width": lax.rem(mw + k, nw)}, device_id_type=MESH)
    for k in sorted(range(1, ns), key=lambda k: abs(min(k, ns - k) - 4)):
        pl.semaphore_signal(barrier, inc=1, device_id={"seq": lax.rem(me + k, ns)}, device_id_type=MESH)

    def at(o, i):
        return pl.ds(o * SUB * pitch + i, SUB, stride=pitch)

    zero = jnp.zeros((SUB, LANES), jnp.float32)
    one = jnp.ones((SUB, LANES), jnp.float32)

    def fill_octet(o):
        def fill(h, _):
            for n in range(SUB // 2):
                n += h * (SUB // 2) + o * SUB
                for j in range(0, seg, 2 * SUB):
                    push_v[pl.ds(n * pitch + j, 2 * SUB), :] = sig_v[
                        pl.ds(pl.multiple_of(n * seg + j, 2 * SUB), 2 * SUB), :].astype(jnp.float32)
            return 0

        lax.fori_loop(0, 2, fill, 0)

    def keep_of(r):
        return jnp.exp2(leak_v[r, :] * (-math.log2(math.e) / total))

    def segment_ends(o):
        half = seg // 2

        def ends_step(i, carry):
            new = []
            for h, (f, b, p) in enumerate(carry):
                r = at(o, i + h * half)
                k = keep_of(r)
                x = push_v[r, :]
                new.append((k * f + x, b + p * x, p * k))
            return tuple(new)

        (f0, b0, p0), (f1, b1, p1) = lax.fori_loop(0, half, ends_step, ((zero, zero, one),) * 2, unroll=16)
        return p1 * f0 + f1, b0 + p0 * b1, p0 * p1

    ends = []
    for o in range(NO):
        loaded(o).wait()
        fill_octet(o)
        ends.append(segment_ends(o))

    def gathered(which):
        return jnp.concatenate([e[which] for e in ends], 0)

    f_end, b_end, p_end = gathered(0), gathered(1), gathered(2)
    row = lax.broadcasted_iota(jnp.int32, (NS, C), 0)

    def shifted(x, d, fill):
        if d > 0:
            return jnp.where(row >= d, pltpu.roll(x, d, 0), fill)
        return jnp.where(row < NS + d, pltpu.roll(x, NS + d, 0), fill)

    pf, ff = p_end, f_end
    pb, bb = p_end, b_end
    d = 1
    while d < NS:
        ff = ff + pf * shifted(ff, d, 0.0)
        pf = pf * shifted(pf, d, 1.0)
        bb = bb + pb * shifted(bb, -d, 0.0)
        pb = pb * shifted(pb, -d, 1.0)
        d *= 2
    tot_v[me] = jnp.concatenate(
        [pf[NS - 1:NS], ff[NS - 1:NS], bb[0:1], jnp.zeros((1, C), jnp.float32)], 0)

    pl.semaphore_wait(barrier, ns + nw - 2)

    def other(k, own):
        return k + jnp.where(k >= own, 1, 0)

    def tot_send(k):
        return pltpu.make_async_remote_copy(
            src_ref=tot_v.at[me], dst_ref=tot_v.at[me], send_sem=ps_sem, recv_sem=tr_sem,
            device_id={"seq": other(k, me)}, device_id_type=MESH)

    def tot_all():
        every = tot_v.at[pl.ds(0, ns - 1)]
        return pltpu.make_async_remote_copy(
            src_ref=every, dst_ref=every, send_sem=ps_sem, recv_sem=tr_sem,
            device_id={"seq": other(0, me)}, device_id_type=MESH)

    for k in range(ns - 1):
        tot_send(k).start()

    def octets_of(x):
        return [x[o * SUB:(o + 1) * SUB] for o in range(NO)]

    f_from, p_from = octets_of(shifted(ff, 1, 0.0)), octets_of(shifted(pf, 1, 1.0))
    b_from, q_from = octets_of(shifted(bb, -1, 0.0)), octets_of(shifted(pb, -1, 1.0))

    def ahead(i, carry):
        new = []
        for o, (f, p) in enumerate(carry):
            r = at(o, i)
            k = keep_of(r)
            f = k * f + push_v[r, :]
            p = p * k
            state_v[r, :] = f
            pre_v[r, :] = p
            new.append((f, p))
        return tuple(new)

    lax.fori_loop(0, seg, ahead, tuple(zip(f_from, p_from)), unroll=4)

    def back(n, carry):
        i = seg - 1 - n
        new = []
        for o, (b, q) in enumerate(carry):
            r = at(o, i)
            k = keep_of(r)
            b = k * b + push_v[r, :]
            q = k * q
            state_v[r, :] = state_v[r, :] + b
            suf_v[r, :] = q
            new.append((b, q))
        return tuple(new)

    lax.fori_loop(0, seg, back, tuple(zip(b_from, q_from)), unroll=4)

    tot_all().wait_recv()
    def folded(which, mask, later_first):
        p = jnp.where(mask, tot_v[:, 0, :], 1.0)
        x = jnp.where(mask, tot_v[:, which, :], 0.0)
        n = ns
        while n > 1:
            d = ns // n
            pl_, xl = pltpu.roll(p, ns - d, 0), pltpu.roll(x, ns - d, 0)
            x = x + p * xl if later_first else pl_ * x + xl
            p = p * pl_
            n //= 2
        return jnp.broadcast_to(x[0:1], (SUB, C))

    who = lax.broadcasted_iota(jnp.int32, (ns, C), 0)
    f_in = folded(1, who < me, False)
    b_in = folded(2, who > me, True)

    ones = jnp.ones((SUB, 2 * LANES), jnp.bfloat16)
    nt = (((1,), (1,)), ((), ()))

    def pow_now(w, h):
        part = pow_v.at[mw, pl.ds(h * SUB, SUB)]
        return pltpu.make_async_remote_copy(
            src_ref=part, dst_ref=part, send_sem=ps_sem, recv_sem=pr_sem, device_id={"width": w}, device_id_type=MESH)

    def pow_bulk(w):
        return pltpu.make_async_remote_copy(
            src_ref=pow_v.at[mw], dst_ref=pow_v.at[mw], send_sem=ps_sem, recv_sem=pr_sem,
            device_id={"width": w}, device_id_type=MESH)

    def bulk_to(k):
        own = jnp.where(mw == 0, 0, jnp.where(mw == 1, nw, mw - 1))
        n = k + jnp.where(k >= own, 1, 0)
        return n + jnp.where(n >= 1, 1, 0)

    def pow_all():
        every = pow_v.at[pl.ds(0, nw - 1)]
        return pltpu.make_async_remote_copy(
            src_ref=every, dst_ref=every, send_sem=ps_sem, recv_sem=pr_sem,
            device_id={"width": other(0, mw)}, device_id_type=MESH)

    def rows_of(b):
        return [pl.ds((b * LANES + j) // seg * pitch + (b * LANES + j) % seg, 2 * SUB) for j in range(0, LANES, 2 * SUB)]

    f16, b16 = jnp.concatenate([f_in] * 2, 0), jnp.concatenate([b_in] * 2, 0)

    def power_stage(carried):
        pending = []

        def store_power(b, res):
            pow_v[mw, pl.ds(b, 1), :] = res[0:1, :LANES]
            pow_v[mw, pl.ds(b + 1, 1), :] = res[0:1, LANES:]
            if (b + 2) % SUB == 0:
                @pl.when(mw != 1)
                def _():
                    pow_now(1, b // SUB).start()

        for b in range(0, NB, 2):
            hi, lo = [], []
            for r in rows_of(b) + rows_of(b + 1):
                st = state_v[r, :] + suf_v[r, :] * b16
                if carried:
                    st = st + pre_v[r, :] * f16
                state_v[r, :] = st
                x = st * st
                h = x.astype(jnp.bfloat16)
                hi.append(h)
                lo.append((x - h.astype(jnp.float32)).astype(jnp.bfloat16))
            both = jnp.concatenate([jnp.concatenate(hi, 0), jnp.concatenate(lo, 0)], 1)
            pending.append((b, lax.dot_general(ones, both, nt, preferred_element_type=jnp.float32)))
            if len(pending) > 1:
                store_power(*pending.pop(0))
        for p in pending:
            store_power(*p)

    @pl.when(me == 0)
    def _():
        power_stage(False)

    @pl.when(me != 0)
    def _():
        power_stage(True)

    for k in range(nw - 2):
        pow_bulk(bulk_to(k)).start()
    @pl.when(mw == 1)
    def _():
        pow_bulk(nw - 1).start()

    gain_copy.wait()
    gain = jnp.broadcast_to(gain_ref[...], (2 * SUB, C))

    def times_gain(s, _):
        for j in range(0, seg, 2 * SUB):
            r = pl.ds(s * pitch + j, 2 * SUB)
            state_v[r, :] = state_v[r, :] * gain
        return 0

    lax.fori_loop(0, NS, times_gain, 0)

    pow_all().wait_recv()
    acc = pow_v[0]
    for w in range(1, nw):
        acc = acc + pow_v[w]
    scale = lax.rsqrt(acc * (1.0 / (C * nw * total)) + 1e-6) * total ** -0.5
    top = scale.astype(jnp.bfloat16).astype(jnp.float32)
    parts = [top, scale - top]
    line = lax.broadcasted_iota(jnp.int32, (LANES, LANES), 0)
    spot = lax.broadcasted_iota(jnp.int32, (LANES, LANES), 1) == line
    every_one = jnp.ones((2 * LANES, LANES), jnp.bfloat16)
    across = [scale[h * SUB:(h + 1) * SUB].T for h in range(NB // SUB)]
    for b in range(NB):
        if b % 2 == 0:
            diag = jnp.concatenate(
                [jnp.where(spot, jnp.broadcast_to(p[b:b + 1], (LANES, LANES)), 0.0).astype(jnp.bfloat16) for p in parts], 1)
            wide = jnp.dot(diag, every_one, preferred_element_type=jnp.float32)
        else:
            wide = jnp.broadcast_to(across[b // SUB][:, b % SUB:b % SUB + 1], (LANES, LANES))
        for q, r in enumerate(rows_of(b)):
            out_v[pl.ds(b * LANES + q * 2 * SUB, 2 * SUB), :] = (
                state_v[r, :] * wide[q * 2 * SUB:(q + 1) * 2 * SUB]).astype(jnp.bfloat16)

    sent = leak_v.at[pl.ds(0, (nw - 1) * NB + (ns - 1) * 4)]
    pltpu.make_async_remote_copy(
        src_ref=sent, dst_ref=sent, send_sem=ps_sem, recv_sem=pr_sem,
        device_id={"width": other(0, mw)}, device_id_type=MESH).wait_send()


def per_device(ns, nw, leak_rate, signal_in, norm_gain):
    _, T, C = leak_rate.shape
    seg = 64
    NS = T // seg
    NO = NS // SUB
    pitch = seg + 4
    f32 = jnp.float32
    vmem = pl.BlockSpec(memory_space=pltpu.VMEM)
    hbm = pl.BlockSpec(memory_space=pl.ANY)
    out = pl.pallas_call(
        functools.partial(join_kernel, ns, nw, seg),
        out_shape=pltpu.VMEM((T, C), jnp.bfloat16),
        in_specs=[hbm, hbm, hbm],
        out_specs=vmem,
        scratch_shapes=[
            pltpu.VMEM((1, C), f32),
            pltpu.VMEM((NS * pitch, C), f32),
            pltpu.VMEM((NS * pitch, C), f32),
            pltpu.VMEM((T, C), jnp.bfloat16),
            pltpu.VMEM((NS * pitch, C), f32),
            pltpu.VMEM((NS * pitch, C), f32),
            pltpu.VMEM((NS * pitch, C), f32),
            pltpu.VMEM((ns, 4, C), f32),
            pltpu.VMEM((nw, T // LANES, LANES), f32),
            pltpu.SemaphoreType.DMA((NO + 1,)),
            pltpu.SemaphoreType.DMA(()),
            pltpu.SemaphoreType.DMA(()),
            pltpu.SemaphoreType.DMA(()),
        ],
        compiler_params=pltpu.CompilerParams(
            collective_id=0, has_side_effects=True, vmem_limit_bytes=32 * 2 ** 20),
    )(pltpu.with_memory_space_constraint(leak_rate[0], pltpu.HBM),
      pltpu.with_memory_space_constraint(signal_in[0], pltpu.HBM),
      pltpu.with_memory_space_constraint(norm_gain[None], pltpu.HBM))
    return out[None]


def solution(mesh):
    return jax.shard_map(
        functools.partial(per_device, mesh.shape["seq"], mesh.shape["width"]),
        mesh=mesh,
        in_specs=(P(None, "seq", "width"), P(None, "seq", "width"), P("width")),
        out_specs=P(None, "seq", "width"),
        check_vma=False,
    )
```

```python
import functools
import math

import jax
import jax.numpy as jnp
from jax import lax
from jax.experimental import pallas as pl
from jax.experimental.pallas import tpu as pltpu
from jax.sharding import PartitionSpec as P

LANES = 128
SUB = 8
MESH = pl.DeviceIdType.MESH


def join_kernel(ns, nw, seg, leak_hbm, sig_hbm, gain_hbm, out_v, gain_ref, state_v, leak_v, sig_v, push_v,
                pre_v, suf_v, own_v, tot_v, pow_v, in_sem, tr_sem, ps_sem, pr_sem):
    T, C = sig_v.shape
    NS = T // seg
    NO = NS // SUB
    NB = T // LANES
    pitch = seg + 4
    rows = SUB * seg
    total = T * ns
    me = lax.axis_index("seq")
    mw = lax.axis_index("width")

    def load(o):
        r = pl.ds(o * rows, rows)
        yield pltpu.make_async_copy(sig_hbm.at[r], sig_v.at[r], in_sem.at[o])
        for n in range(o * SUB, (o + 1) * SUB):
            yield pltpu.make_async_copy(
                leak_hbm.at[pl.ds(n * seg, seg)], leak_v.at[pl.ds(n * pitch, seg)], in_sem.at[o])

    def loaded(o):
        every = pl.ds(0, rows + rows // 2 + (1 if o == NO - 1 else 0))
        return pltpu.make_async_copy(leak_hbm.at[every], leak_v.at[every], in_sem.at[o])

    for o in range(NO):
        for c in load(o):
            c.start()

    pltpu.make_async_copy(gain_hbm, gain_ref, in_sem.at[NO - 1]).start()

    barrier = pltpu.get_barrier_semaphore()
    for k in sorted(range(1, nw), key=lambda k: abs(min(k, nw - k) - 3 * nw // 8)):
        pl.semaphore_signal(barrier, inc=1, device_id={"width": lax.rem(mw + k, nw)}, device_id_type=MESH)
    for k in sorted(range(1, ns), key=lambda k: abs(min(k, ns - k) - 4)):
        pl.semaphore_signal(barrier, inc=1, device_id={"seq": lax.rem(me + k, ns)}, device_id_type=MESH)

    def at(o, i):
        return pl.ds(o * SUB * pitch + i, SUB, stride=pitch)

    zero = jnp.zeros((SUB, LANES), jnp.float32)
    one = jnp.ones((SUB, LANES), jnp.float32)

    def fill_octet(o):
        def fill(h, _):
            for n in range(SUB // 2):
                n += h * (SUB // 2) + o * SUB
                for j in range(0, seg, 2 * SUB):
                    push_v[pl.ds(n * pitch + j, 2 * SUB), :] = sig_v[
                        pl.ds(pl.multiple_of(n * seg + j, 2 * SUB), 2 * SUB), :].astype(jnp.float32)
            return 0

        lax.fori_loop(0, 2, fill, 0)

    def keep_of(r):
        return jnp.exp2(leak_v[r, :] * (-math.log2(math.e) / total))

    def segment_ends(o):
        half = seg // 2

        def ends_step(i, carry):
            new = []
            for h, (f, b, p) in enumerate(carry):
                r = at(o, i + h * half)
                k = keep_of(r)
                x = push_v[r, :]
                new.append((k * f + x, b + p * x, p * k))
            return tuple(new)

        (f0, b0, p0), (f1, b1, p1) = lax.fori_loop(0, half, ends_step, ((zero, zero, one),) * 2, unroll=16)
        return p1 * f0 + f1, b0 + p0 * b1, p0 * p1

    ends = []
    for o in range(NO):
        loaded(o).wait()
        fill_octet(o)
        ends.append(segment_ends(o))

    def gathered(which):
        return jnp.concatenate([e[which] for e in ends], 0)

    f_end, b_end, p_end = gathered(0), gathered(1), gathered(2)
    row = lax.broadcasted_iota(jnp.int32, (NS, C), 0)

    def shifted(x, d, fill):
        if d > 0:
            return jnp.where(row >= d, pltpu.roll(x, d, 0), fill)
        return jnp.where(row < NS + d, pltpu.roll(x, NS + d, 0), fill)

    pf, ff = p_end, f_end
    pb, bb = p_end, b_end
    d = 1
    while d < NS:
        ff = ff + pf * shifted(ff, d, 0.0)
        pf = pf * shifted(pf, d, 1.0)
        bb = bb + pb * shifted(bb, -d, 0.0)
        pb = pb * shifted(pb, -d, 1.0)
        d *= 2
    own_v[...] = jnp.concatenate(
        [pf[NS - 1:NS], ff[NS - 1:NS], bb[0:1], jnp.zeros((1, C), jnp.float32)], 0)
    for n in range(3):
        tot_v[n, pl.ds(me, 1)] = jnp.zeros((1, C), jnp.float32)

    pl.semaphore_wait(barrier, ns + nw - 2)

    def other(k, own):
        return k + jnp.where(k >= own, 1, 0)

    def tot_send(k):
        return pltpu.make_async_remote_copy(
            src_ref=own_v, dst_ref=tot_v.at[:, me], send_sem=ps_sem, recv_sem=tr_sem,
            device_id={"seq": other(k, me)}, device_id_type=MESH)

    def tot_all():
        every = tot_v.at[:, pl.ds(0, ns - 1)]
        return pltpu.make_async_remote_copy(
            src_ref=every, dst_ref=every, send_sem=ps_sem, recv_sem=tr_sem,
            device_id={"seq": other(0, me)}, device_id_type=MESH)

    for k in range(ns - 1):
        tot_send(k).start()

    def octets_of(x):
        return [x[o * SUB:(o + 1) * SUB] for o in range(NO)]

    f_from, p_from = octets_of(shifted(ff, 1, 0.0)), octets_of(shifted(pf, 1, 1.0))
    b_from, q_from = octets_of(shifted(bb, -1, 0.0)), octets_of(shifted(pb, -1, 1.0))

    def ahead(i, carry):
        new = []
        for o, (f, p) in enumerate(carry):
            r = at(o, i)
            k = keep_of(r)
            f = k * f + push_v[r, :]
            p = p * k
            state_v[r, :] = f
            pre_v[r, :] = p
            new.append((f, p))
        return tuple(new)

    lax.fori_loop(0, seg, ahead, tuple(zip(f_from, p_from)), unroll=4)

    def back(n, carry):
        i = seg - 1 - n
        new = []
        for o, (b, q) in enumerate(carry):
            r = at(o, i)
            k = keep_of(r)
            b = k * b + push_v[r, :]
            q = k * q
            state_v[r, :] = state_v[r, :] + b
            suf_v[r, :] = q
            new.append((b, q))
        return tuple(new)

    lax.fori_loop(0, seg, back, tuple(zip(b_from, q_from)), unroll=4)

    tot_all().wait_recv()
    def folded(which, mask, later_first):
        p = jnp.where(mask, tot_v[0], 1.0)
        x = jnp.where(mask, tot_v[which], 0.0)
        n = ns
        while n > 1:
            d = ns // n
            pl_, xl = pltpu.roll(p, ns - d, 0), pltpu.roll(x, ns - d, 0)
            x = x + p * xl if later_first else pl_ * x + xl
            p = p * pl_
            n //= 2
        return jnp.broadcast_to(x[0:1], (SUB, C))

    who = lax.broadcasted_iota(jnp.int32, (ns, C), 0)
    f_in = folded(1, who < me, False)
    b_in = folded(2, who > me, True)

    ones = jnp.ones((SUB, 2 * LANES), jnp.bfloat16)
    nt = (((1,), (1,)), ((), ()))

    def pow_now(w, h):
        part = pow_v.at[mw, pl.ds(h * SUB, SUB)]
        return pltpu.make_async_remote_copy(
            src_ref=part, dst_ref=part, send_sem=ps_sem, recv_sem=pr_sem, device_id={"width": w}, device_id_type=MESH)

    def pow_bulk(w):
        return pltpu.make_async_remote_copy(
            src_ref=pow_v.at[mw], dst_ref=pow_v.at[mw], send_sem=ps_sem, recv_sem=pr_sem,
            device_id={"width": w}, device_id_type=MESH)

    def bulk_to(k):
        own = jnp.where(mw == 0, 0, jnp.where(mw == 1, nw, mw - 1))
        n = k + jnp.where(k >= own, 1, 0)
        return n + jnp.where(n >= 1, 1, 0)

    def pow_all():
        every = pow_v.at[pl.ds(0, nw - 1)]
        return pltpu.make_async_remote_copy(
            src_ref=every, dst_ref=every, send_sem=ps_sem, recv_sem=pr_sem,
            device_id={"width": other(0, mw)}, device_id_type=MESH)

    def rows_of(b):
        return [pl.ds((b * LANES + j) // seg * pitch + (b * LANES + j) % seg, 2 * SUB) for j in range(0, LANES, 2 * SUB)]

    f16, b16 = jnp.concatenate([f_in] * 2, 0), jnp.concatenate([b_in] * 2, 0)

    def power_stage(carried):
        pending, depth = [], 3

        def store_power(b, res):
            pow_v[mw, pl.ds(b, 1), :] = res[0:1, :LANES]
            pow_v[mw, pl.ds(b + 1, 1), :] = res[0:1, LANES:]
            if (b + 2) % SUB == 0:
                @pl.when(mw != 1)
                def _():
                    pow_now(1, b // SUB).start()

        for b in range(0, NB, 2):
            hi, lo = [], []
            for r in rows_of(b) + rows_of(b + 1):
                st = state_v[r, :] + suf_v[r, :] * b16
                if carried:
                    st = st + pre_v[r, :] * f16
                state_v[r, :] = st
                x = st * st
                h = x.astype(jnp.bfloat16)
                hi.append(h)
                lo.append((x - h.astype(jnp.float32)).astype(jnp.bfloat16))
            both = jnp.concatenate([jnp.concatenate(hi, 0), jnp.concatenate(lo, 0)], 1)
            pending.append((b, lax.dot_general(ones, both, nt, preferred_element_type=jnp.float32)))
            if len(pending) > depth:
                store_power(*pending.pop(0))
        for p in pending:
            store_power(*p)

    @pl.when(me == 0)
    def _():
        power_stage(False)

    @pl.when(me != 0)
    def _():
        power_stage(True)

    for k in range(nw - 2):
        pow_bulk(bulk_to(k)).start()
    @pl.when(mw == 1)
    def _():
        pow_bulk(nw - 1).start()

    gain = jnp.broadcast_to(gain_ref[...], (2 * SUB, C))

    def times_gain(s, _):
        for j in range(0, seg, 2 * SUB):
            r = pl.ds(s * pitch + j, 2 * SUB)
            state_v[r, :] = state_v[r, :] * gain
        return 0

    lax.fori_loop(0, NS, times_gain, 0)

    pow_all().wait_recv()
    acc = pow_v[0]
    for w in range(1, nw):
        acc = acc + pow_v[w]
    scale = lax.rsqrt(acc * (1.0 / (C * nw * total)) + 1e-6) * total ** -0.5
    top = scale.astype(jnp.bfloat16).astype(jnp.float32)
    parts = [top, scale - top]
    line = lax.broadcasted_iota(jnp.int32, (LANES, LANES), 0)
    spot = lax.broadcasted_iota(jnp.int32, (LANES, LANES), 1) == line
    every_one = jnp.ones((2 * LANES, LANES), jnp.bfloat16)
    across = [scale[h * SUB:(h + 1) * SUB].T for h in range(NB // SUB)]
    def diagonal(b):
        return jnp.concatenate(
            [jnp.where(spot, jnp.broadcast_to(p[b:b + 1], (LANES, LANES)), 0.0).astype(jnp.bfloat16) for p in parts], 1)

    def finish(b, wide):
        for q, r in enumerate(rows_of(b)):
            out_v[pl.ds(b * LANES + q * 2 * SUB, 2 * SUB), :] = (
                state_v[r, :] * wide[q * 2 * SUB:(q + 1) * 2 * SUB]).astype(jnp.bfloat16)

    by_dot, group = 10, 5
    for a in range(0, by_dot, group):
        wide = jnp.dot(jnp.concatenate([diagonal(b) for b in range(a, a + group)], 0), every_one,
                       preferred_element_type=jnp.float32)
        for b in range(a, a + group):
            finish(b, wide[(b - a) * LANES:(b - a + 1) * LANES])
    for b in range(by_dot, NB):
        finish(b, jnp.broadcast_to(across[b // SUB][:, b % SUB:b % SUB + 1], (LANES, LANES)))

    sent = leak_v.at[pl.ds(0, (nw - 1) * NB + (ns - 1) * 4)]
    pltpu.make_async_remote_copy(
        src_ref=sent, dst_ref=sent, send_sem=ps_sem, recv_sem=pr_sem,
        device_id={"width": other(0, mw)}, device_id_type=MESH).wait_send()


def per_device(ns, nw, leak_rate, signal_in, norm_gain):
    _, T, C = leak_rate.shape
    seg = 64
    NS = T // seg
    NO = NS // SUB
    pitch = seg + 4
    f32 = jnp.float32
    vmem = pl.BlockSpec(memory_space=pltpu.VMEM)
    hbm = pl.BlockSpec(memory_space=pl.ANY)
    out = pl.pallas_call(
        functools.partial(join_kernel, ns, nw, seg),
        out_shape=pltpu.VMEM((T, C), jnp.bfloat16),
        in_specs=[hbm, hbm, hbm],
        out_specs=vmem,
        scratch_shapes=[
            pltpu.VMEM((1, C), f32),
            pltpu.VMEM((NS * pitch, C), f32),
            pltpu.VMEM((NS * pitch, C), f32),
            pltpu.VMEM((T, C), jnp.bfloat16),
            pltpu.VMEM((NS * pitch, C), f32),
            pltpu.VMEM((NS * pitch, C), f32),
            pltpu.VMEM((NS * pitch, C), f32),
            pltpu.VMEM((4, C), f32),
            pltpu.VMEM((4, ns, C), f32),
            pltpu.VMEM((nw, T // LANES, LANES), f32),
            pltpu.SemaphoreType.DMA((NO,)),
            pltpu.SemaphoreType.DMA(()),
            pltpu.SemaphoreType.DMA(()),
            pltpu.SemaphoreType.DMA(()),
        ],
        compiler_params=pltpu.CompilerParams(
            collective_id=0, has_side_effects=True, vmem_limit_bytes=32 * 2 ** 20),
    )(pltpu.with_memory_space_constraint(leak_rate[0], pltpu.HBM),
      pltpu.with_memory_space_constraint(signal_in[0], pltpu.HBM),
      pltpu.with_memory_space_constraint(norm_gain[None], pltpu.HBM))
    return out[None]


def solution(mesh):
    return jax.shard_map(
        functools.partial(per_device, mesh.shape["seq"], mesh.shape["width"]),
        mesh=mesh,
        in_specs=(P(None, "seq", "width"), P(None, "seq", "width"), P("width")),
        out_specs=P(None, "seq", "width"),
        check_vma=False,
    )
```

```python
import functools
import math

import jax
import jax.numpy as jnp
from jax import lax
from jax.experimental import pallas as pl
from jax.experimental.pallas import tpu as pltpu
from jax.sharding import PartitionSpec as P

LANES = 128
GROUPS = ((4, 4), (2, 6))
SUB = 8
MESH = pl.DeviceIdType.MESH


def join_kernel(ns, nw, seg, leak_hbm, sig_hbm, gain_hbm, state_v, pow_v, gain_ref, leak_v, sig_v, push_v,
                pre_v, suf_v, own_v, tot_v, in_sem, tr_sem, ps_sem, pr_sem):
    T, C = sig_v.shape
    NS = T // seg
    NO = NS // SUB
    NB = T // LANES
    pitch = seg + 4
    rows = SUB * seg
    total = T * ns
    me = lax.axis_index("seq")
    mw = lax.axis_index("width")

    def load(o):
        r = pl.ds(o * rows, rows)
        yield pltpu.make_async_copy(sig_hbm.at[r], sig_v.at[r], in_sem.at[o])
        for n in range(o * SUB, (o + 1) * SUB):
            yield pltpu.make_async_copy(
                leak_hbm.at[pl.ds(n * seg, seg)], leak_v.at[pl.ds(n * pitch, seg)], in_sem.at[o])

    def loaded(o):
        every = pl.ds(0, rows + rows // 2 + (1 if o == NO - 1 else 0))
        return pltpu.make_async_copy(leak_hbm.at[every], leak_v.at[every], in_sem.at[o])

    for o in range(NO):
        for c in load(o):
            c.start()

    pltpu.make_async_copy(gain_hbm, gain_ref, in_sem.at[NO - 1]).start()

    barrier = pltpu.get_barrier_semaphore()
    for k in sorted(range(1, nw), key=lambda k: abs(min(k, nw - k) - 3 * nw // 8)):
        pl.semaphore_signal(barrier, inc=1, device_id={"width": lax.rem(mw + k, nw)}, device_id_type=MESH)
    for k in sorted(range(1, ns), key=lambda k: abs(min(k, ns - k) - 4)):
        pl.semaphore_signal(barrier, inc=1, device_id={"seq": lax.rem(me + k, ns)}, device_id_type=MESH)

    def at(o, i):
        return pl.ds(o * SUB * pitch + i, SUB, stride=pitch)

    zero = jnp.zeros((SUB, LANES), jnp.float32)
    one = jnp.ones((SUB, LANES), jnp.float32)

    def fill_octet(o):
        def fill(h, _):
            for n in range(SUB // 2):
                n += h * (SUB // 2) + o * SUB
                for j in range(0, seg, 2 * SUB):
                    push_v[pl.ds(n * pitch + j, 2 * SUB), :] = sig_v[
                        pl.ds(pl.multiple_of(n * seg + j, 2 * SUB), 2 * SUB), :].astype(jnp.float32)
            return 0

        lax.fori_loop(0, 2, fill, 0)

    def keep_of(r):
        return jnp.exp2(leak_v[r, :] * (-math.log2(math.e) / total))

    def segment_ends(o):
        half = seg // 2

        def ends_step(i, carry):
            new = []
            for h, (f, b, p) in enumerate(carry):
                r = at(o, i + h * half)
                k = keep_of(r)
                x = push_v[r, :]
                new.append((k * f + x, b + p * x, p * k))
            return tuple(new)

        (f0, b0, p0), (f1, b1, p1) = lax.fori_loop(0, half, ends_step, ((zero, zero, one),) * 2, unroll=16)
        return p1 * f0 + f1, b0 + p0 * b1, p0 * p1

    ends = []
    for o in range(NO):
        loaded(o).wait()
        fill_octet(o)
        ends.append(segment_ends(o))

    def gathered(which):
        return jnp.concatenate([e[which] for e in ends], 0)

    f_end, b_end, p_end = gathered(0), gathered(1), gathered(2)
    row = lax.broadcasted_iota(jnp.int32, (NS, C), 0)

    def shifted(x, d, fill):
        if d > 0:
            return jnp.where(row >= d, pltpu.roll(x, d, 0), fill)
        return jnp.where(row < NS + d, pltpu.roll(x, NS + d, 0), fill)

    pf, ff = p_end, f_end
    pb, bb = p_end, b_end
    d = 1
    while d < NS:
        ff = ff + pf * shifted(ff, d, 0.0)
        pf = pf * shifted(pf, d, 1.0)
        bb = bb + pb * shifted(bb, -d, 0.0)
        pb = pb * shifted(pb, -d, 1.0)
        d *= 2
    own_v[...] = jnp.concatenate(
        [pf[NS - 1:NS], ff[NS - 1:NS], bb[0:1], jnp.zeros((1, C), jnp.float32)], 0)
    for n in range(3):
        tot_v[n, pl.ds(me, 1)] = jnp.zeros((1, C), jnp.float32)

    pl.semaphore_wait(barrier, ns + nw - 2)

    def other(k, own):
        return k + jnp.where(k >= own, 1, 0)

    def tot_send(k):
        return pltpu.make_async_remote_copy(
            src_ref=own_v, dst_ref=tot_v.at[:, me], send_sem=ps_sem, recv_sem=tr_sem,
            device_id={"seq": other(k, me)}, device_id_type=MESH)

    def tot_all():
        every = tot_v.at[:, pl.ds(0, ns - 1)]
        return pltpu.make_async_remote_copy(
            src_ref=every, dst_ref=every, send_sem=ps_sem, recv_sem=tr_sem,
            device_id={"seq": other(0, me)}, device_id_type=MESH)

    for k in range(ns - 1):
        tot_send(k).start()

    def octets_of(x):
        return [x[o * SUB:(o + 1) * SUB] for o in range(NO)]

    f_from, p_from = octets_of(shifted(ff, 1, 0.0)), octets_of(shifted(pf, 1, 1.0))
    b_from, q_from = octets_of(shifted(bb, -1, 0.0)), octets_of(shifted(pb, -1, 1.0))

    def ahead(i, carry):
        new = []
        for o, (f, p) in enumerate(carry):
            r = at(o, i)
            k = keep_of(r)
            f = k * f + push_v[r, :]
            p = p * k
            state_v[r, :] = f
            pre_v[r, :] = p
            new.append((f, p))
        return tuple(new)

    lax.fori_loop(0, seg, ahead, tuple(zip(f_from, p_from)), unroll=4)

    def back(n, carry):
        i = seg - 1 - n
        new = []
        for o, (b, q) in enumerate(carry):
            r = at(o, i)
            k = keep_of(r)
            b = k * b + push_v[r, :]
            q = k * q
            state_v[r, :] = state_v[r, :] + b
            suf_v[r, :] = q
            new.append((b, q))
        return tuple(new)

    lax.fori_loop(0, seg, back, tuple(zip(b_from, q_from)), unroll=4)

    tot_all().wait_recv()
    def folded(which, mask, later_first):
        p = jnp.where(mask, tot_v[0], 1.0)
        x = jnp.where(mask, tot_v[which], 0.0)
        n = ns
        while n > 1:
            d = ns // n
            pl_, xl = pltpu.roll(p, ns - d, 0), pltpu.roll(x, ns - d, 0)
            x = x + p * xl if later_first else pl_ * x + xl
            p = p * pl_
            n //= 2
        return jnp.broadcast_to(x[0:1], (SUB, C))

    who = lax.broadcasted_iota(jnp.int32, (ns, C), 0)
    f_in = folded(1, who < me, False)
    b_in = folded(2, who > me, True)

    ones = jnp.ones((SUB, 2 * LANES), jnp.bfloat16)
    nt = (((1,), (1,)), ((), ()))

    def pow_now(w, h):
        part = pow_v.at[mw, pl.ds(h * SUB, SUB)]
        return pltpu.make_async_remote_copy(
            src_ref=part, dst_ref=part, send_sem=ps_sem, recv_sem=pr_sem, device_id={"width": w}, device_id_type=MESH)

    def pow_bulk(w):
        return pltpu.make_async_remote_copy(
            src_ref=pow_v.at[mw], dst_ref=pow_v.at[mw], send_sem=ps_sem, recv_sem=pr_sem,
            device_id={"width": w}, device_id_type=MESH)

    def bulk_to(k):
        own = jnp.where(mw == 0, 0, jnp.where(mw == 1, nw, mw - 1))
        n = k + jnp.where(k >= own, 1, 0)
        return n + jnp.where(n >= 1, 1, 0)

    def pow_all():
        every = pow_v.at[pl.ds(0, nw - 1)]
        return pltpu.make_async_remote_copy(
            src_ref=every, dst_ref=every, send_sem=ps_sem, recv_sem=pr_sem,
            device_id={"width": other(0, mw)}, device_id_type=MESH)

    def rows_of(b):
        return [pl.ds((b * LANES + j) // seg * pitch + (b * LANES + j) % seg, 2 * SUB) for j in range(0, LANES, 2 * SUB)]

    f16, b16 = jnp.concatenate([f_in] * 2, 0), jnp.concatenate([b_in] * 2, 0)

    def power_stage(carried):
        pending, depth = [], 3

        def store_power(b, res):
            pow_v[mw, pl.ds(b, 1), :] = res[0:1, :LANES]
            pow_v[mw, pl.ds(b + 1, 1), :] = res[0:1, LANES:]
            if (b + 2) % SUB == 0:
                @pl.when(mw != 1)
                def _():
                    pow_now(1, b // SUB).start()

        for b in range(0, NB, 2):
            hi, lo = [], []
            for r in rows_of(b) + rows_of(b + 1):
                st = state_v[r, :] + suf_v[r, :] * b16
                if carried:
                    st = st + pre_v[r, :] * f16
                state_v[r, :] = st
                x = st * st
                h = x.astype(jnp.bfloat16)
                hi.append(h)
                lo.append((x - h.astype(jnp.float32)).astype(jnp.bfloat16))
            both = jnp.concatenate([jnp.concatenate(hi, 0), jnp.concatenate(lo, 0)], 1)
            pending.append((b, lax.dot_general(ones, both, nt, preferred_element_type=jnp.float32)))
            if len(pending) > depth:
                store_power(*pending.pop(0))
        for p in pending:
            store_power(*p)

    @pl.when(me == 0)
    def _():
        power_stage(False)

    @pl.when(me != 0)
    def _():
        power_stage(True)

    for k in range(nw - 2):
        pow_bulk(bulk_to(k)).start()
    @pl.when(mw == 1)
    def _():
        pow_bulk(nw - 1).start()

    gain = jnp.broadcast_to(gain_ref[...], (2 * SUB, C))

    def times_gain(s, _):
        for j in range(0, seg, 2 * SUB):
            r = pl.ds(s * pitch + j, 2 * SUB)
            state_v[r, :] = state_v[r, :] * gain
        return 0

    lax.fori_loop(0, NS, times_gain, 0)

    pow_all().wait_recv()
    sent = leak_v.at[pl.ds(0, (nw - 1) * NB + (ns - 1) * 4)]
    pltpu.make_async_remote_copy(
        src_ref=sent, dst_ref=sent, send_sem=ps_sem, recv_sem=pr_sem,
        device_id={"width": other(0, mw)}, device_id_type=MESH).wait_send()


def close_kernel(ns, nw, seg, groups, state_v, pow_v, out_hbm, out_v, sem):
    T, C = out_v.shape
    NB = T // LANES
    pitch = seg + 4
    total = T * ns

    def rows_of(b):
        return [pl.ds((b * LANES + j) // seg * pitch + (b * LANES + j) % seg, 2 * SUB) for j in range(0, LANES, 2 * SUB)]

    acc = pow_v[0]
    for w in range(1, nw):
        acc = acc + pow_v[w]
    scale = lax.rsqrt(acc * (1.0 / (C * nw * total)) + 1e-6) * total ** -0.5
    top = scale.astype(jnp.bfloat16).astype(jnp.float32)
    parts = [top, scale - top]
    line = lax.broadcasted_iota(jnp.int32, (LANES, LANES), 0)
    spot = lax.broadcasted_iota(jnp.int32, (LANES, LANES), 1) == line
    every_one = jnp.ones((2 * LANES, LANES), jnp.bfloat16)
    across = [scale[h * SUB:(h + 1) * SUB].T for h in range(NB // SUB)]
    def diagonal(b):
        return jnp.concatenate(
            [jnp.where(spot, jnp.broadcast_to(p[b:b + 1], (LANES, LANES)), 0.0).astype(jnp.bfloat16) for p in parts], 1)

    def finish(b, wide):
        for q, r in enumerate(rows_of(b)):
            out_v[pl.ds(b * LANES + q * 2 * SUB, 2 * SUB), :] = (
                state_v[r, :] * wide[q * 2 * SUB:(q + 1) * 2 * SUB]).astype(jnp.bfloat16)

    def by_lanes(b):
        return jnp.broadcast_to(across[b // SUB][:, b % SUB:b % SUB + 1], (LANES, LANES))

    def by_dots(bs):
        wide = jnp.dot(jnp.concatenate([diagonal(b) for b in bs], 0), every_one, preferred_element_type=jnp.float32)
        return [wide[n * LANES:(n + 1) * LANES] for n in range(len(bs))]

    first = 0
    for n, (lanes, dots) in enumerate(groups):
        bs = list(range(first, first + lanes + dots))
        wides = [by_lanes(b) for b in bs[:lanes]] + (by_dots(bs[lanes:]) if dots else [])
        for b, w in zip(bs, wides):
            finish(b, w)
        r = pl.ds(first * LANES, len(bs) * LANES)
        pltpu.make_async_copy(out_v.at[r], out_hbm.at[r], sem).start()
        first += len(bs)
    pltpu.make_async_copy(out_v, out_hbm, sem).wait()


def per_device(ns, nw, leak_rate, signal_in, norm_gain):
    _, T, C = leak_rate.shape
    seg = 64
    NS = T // seg
    NO = NS // SUB
    pitch = seg + 4
    f32 = jnp.float32
    vmem = pl.BlockSpec(memory_space=pltpu.VMEM)
    hbm = pl.BlockSpec(memory_space=pl.ANY)
    state, power = pl.pallas_call(
        functools.partial(join_kernel, ns, nw, seg),
        out_shape=(pltpu.VMEM((NS * pitch, C), f32), pltpu.VMEM((nw, T // LANES, LANES), f32)),
        in_specs=[hbm, hbm, hbm],
        out_specs=(vmem, vmem),
        scratch_shapes=[
            pltpu.VMEM((1, C), f32),
            pltpu.VMEM((NS * pitch, C), f32),
            pltpu.VMEM((T, C), jnp.bfloat16),
            pltpu.VMEM((NS * pitch, C), f32),
            pltpu.VMEM((NS * pitch, C), f32),
            pltpu.VMEM((NS * pitch, C), f32),
            pltpu.VMEM((4, C), f32),
            pltpu.VMEM((4, ns, C), f32),
            pltpu.SemaphoreType.DMA((NO,)),
            pltpu.SemaphoreType.DMA(()),
            pltpu.SemaphoreType.DMA(()),
            pltpu.SemaphoreType.DMA(()),
        ],
        compiler_params=pltpu.CompilerParams(
            collective_id=0, has_side_effects=True, vmem_limit_bytes=32 * 2 ** 20),
    )(pltpu.with_memory_space_constraint(leak_rate[0], pltpu.HBM),
      pltpu.with_memory_space_constraint(signal_in[0], pltpu.HBM),
      pltpu.with_memory_space_constraint(norm_gain[None], pltpu.HBM))
    out = pl.pallas_call(
        functools.partial(close_kernel, ns, nw, seg, GROUPS),
        out_shape=pltpu.HBM((T, C), jnp.bfloat16),
        in_specs=[vmem, vmem],
        out_specs=hbm,
        scratch_shapes=[pltpu.VMEM((T, C), jnp.bfloat16), pltpu.SemaphoreType.DMA(())],
        compiler_params=pltpu.CompilerParams(vmem_limit_bytes=32 * 2 ** 20),
    )(state, power)
    return out[None]


def solution(mesh):
    return jax.shard_map(
        functools.partial(per_device, mesh.shape["seq"], mesh.shape["width"]),
        mesh=mesh,
        in_specs=(P(None, "seq", "width"), P(None, "seq", "width"), P("width")),
        out_specs=P(None, "seq", "width"),
        check_vma=False,
    )
```

```python
import functools
import math

import jax
import jax.numpy as jnp
from jax import lax
from jax.experimental import pallas as pl
from jax.experimental.pallas import tpu as pltpu
from jax.sharding import PartitionSpec as P

LANES = 128
GROUPS = ((2, 3), (2, 3), (1, 3), (1, 1))
SUB = 8
MESH = pl.DeviceIdType.MESH


def join_kernel(ns, nw, seg, leak_hbm, sig_hbm, gain_hbm, state_v, pow_v, gain_ref, leak_v, sig_v, push_v,
                pre_v, suf_v, own_v, tot_v, in_sem, tr_sem, ps_sem, pr_sem):
    T, C = sig_v.shape
    NS = T // seg
    NO = NS // SUB
    NB = T // LANES
    pitch = seg + 4
    rows = SUB * seg
    total = T * ns
    me = lax.axis_index("seq")
    mw = lax.axis_index("width")

    def load(o):
        r = pl.ds(o * rows, rows)
        yield pltpu.make_async_copy(sig_hbm.at[r], sig_v.at[r], in_sem.at[o])
        for n in range(o * SUB, (o + 1) * SUB):
            yield pltpu.make_async_copy(
                leak_hbm.at[pl.ds(n * seg, seg)], leak_v.at[pl.ds(n * pitch, seg)], in_sem.at[o])

    def loaded(o):
        every = pl.ds(0, rows + rows // 2 + (1 if o == NO - 1 else 0))
        return pltpu.make_async_copy(leak_hbm.at[every], leak_v.at[every], in_sem.at[o])

    for o in range(NO):
        for c in load(o):
            c.start()

    pltpu.make_async_copy(gain_hbm, gain_ref, in_sem.at[NO - 1]).start()

    barrier = pltpu.get_barrier_semaphore()
    for k in sorted(range(1, nw), key=lambda k: abs(min(k, nw - k) - 3 * nw // 8)):
        pl.semaphore_signal(barrier, inc=1, device_id={"width": lax.rem(mw + k, nw)}, device_id_type=MESH)
    for k in sorted(range(1, ns), key=lambda k: abs(min(k, ns - k) - 4)):
        pl.semaphore_signal(barrier, inc=1, device_id={"seq": lax.rem(me + k, ns)}, device_id_type=MESH)

    def at(o, i):
        return pl.ds(o * SUB * pitch + i, SUB, stride=pitch)

    zero = jnp.zeros((SUB, LANES), jnp.float32)
    one = jnp.ones((SUB, LANES), jnp.float32)

    def fill_octet(o):
        def fill(h, _):
            for n in range(SUB // 2):
                n += h * (SUB // 2) + o * SUB
                for j in range(0, seg, 2 * SUB):
                    push_v[pl.ds(n * pitch + j, 2 * SUB), :] = sig_v[
                        pl.ds(pl.multiple_of(n * seg + j, 2 * SUB), 2 * SUB), :].astype(jnp.float32)
            return 0

        lax.fori_loop(0, 2, fill, 0)

    def keep_of(r):
        return jnp.exp2(leak_v[r, :] * (-math.log2(math.e) / total))

    def segment_ends(o):
        half = seg // 2

        def ends_step(i, carry):
            new = []
            for h, (f, b, p) in enumerate(carry):
                r = at(o, i + h * half)
                k = keep_of(r)
                x = push_v[r, :]
                new.append((k * f + x, b + p * x, p * k))
            return tuple(new)

        (f0, b0, p0), (f1, b1, p1) = lax.fori_loop(0, half, ends_step, ((zero, zero, one),) * 2, unroll=16)
        return p1 * f0 + f1, b0 + p0 * b1, p0 * p1

    ends = []
    for o in range(NO):
        loaded(o).wait()
        fill_octet(o)
        ends.append(segment_ends(o))

    def gathered(which):
        return jnp.concatenate([e[which] for e in ends], 0)

    f_end, b_end, p_end = gathered(0), gathered(1), gathered(2)
    row = lax.broadcasted_iota(jnp.int32, (NS, C), 0)

    def shifted(x, d, fill):
        if d > 0:
            return jnp.where(row >= d, pltpu.roll(x, d, 0), fill)
        return jnp.where(row < NS + d, pltpu.roll(x, NS + d, 0), fill)

    pf, ff = p_end, f_end
    pb, bb = p_end, b_end
    d = 1
    while d < NS:
        ff = ff + pf * shifted(ff, d, 0.0)
        pf = pf * shifted(pf, d, 1.0)
        bb = bb + pb * shifted(bb, -d, 0.0)
        pb = pb * shifted(pb, -d, 1.0)
        d *= 2
    own_v[...] = jnp.concatenate(
        [pf[NS - 1:NS], ff[NS - 1:NS], bb[0:1], jnp.zeros((1, C), jnp.float32)], 0)
    for n in range(3):
        tot_v[n, pl.ds(me, 1)] = jnp.zeros((1, C), jnp.float32)

    pl.semaphore_wait(barrier, ns + nw - 2)

    def other(k, own):
        return k + jnp.where(k >= own, 1, 0)

    def tot_send(k):
        return pltpu.make_async_remote_copy(
            src_ref=own_v, dst_ref=tot_v.at[:, me], send_sem=ps_sem, recv_sem=tr_sem,
            device_id={"seq": other(k, me)}, device_id_type=MESH)

    def tot_all():
        every = tot_v.at[:, pl.ds(0, ns - 1)]
        return pltpu.make_async_remote_copy(
            src_ref=every, dst_ref=every, send_sem=ps_sem, recv_sem=tr_sem,
            device_id={"seq": other(0, me)}, device_id_type=MESH)

    for k in range(ns - 1):
        tot_send(k).start()

    def octets_of(x):
        return [x[o * SUB:(o + 1) * SUB] for o in range(NO)]

    f_from, p_from = octets_of(shifted(ff, 1, 0.0)), octets_of(shifted(pf, 1, 1.0))
    b_from, q_from = octets_of(shifted(bb, -1, 0.0)), octets_of(shifted(pb, -1, 1.0))

    def ahead(i, carry):
        new = []
        for o, (f, p) in enumerate(carry):
            r = at(o, i)
            k = keep_of(r)
            f = k * f + push_v[r, :]
            p = p * k
            state_v[r, :] = f
            pre_v[r, :] = p
            new.append((f, p))
        return tuple(new)

    lax.fori_loop(0, seg, ahead, tuple(zip(f_from, p_from)), unroll=4)

    def back(n, carry):
        i = seg - 1 - n
        new = []
        for o, (b, q) in enumerate(carry):
            r = at(o, i)
            k = keep_of(r)
            b = k * b + push_v[r, :]
            q = k * q
            state_v[r, :] = state_v[r, :] + b
            suf_v[r, :] = q
            new.append((b, q))
        return tuple(new)

    lax.fori_loop(0, seg, back, tuple(zip(b_from, q_from)), unroll=4)

    tot_all().wait_recv()
    def folded(which, mask, later_first):
        p = jnp.where(mask, tot_v[0], 1.0)
        x = jnp.where(mask, tot_v[which], 0.0)
        n = ns
        while n > 1:
            d = ns // n
            pl_, xl = pltpu.roll(p, ns - d, 0), pltpu.roll(x, ns - d, 0)
            x = x + p * xl if later_first else pl_ * x + xl
            p = p * pl_
            n //= 2
        return jnp.broadcast_to(x[0:1], (SUB, C))

    who = lax.broadcasted_iota(jnp.int32, (ns, C), 0)
    f_in = folded(1, who < me, False)
    b_in = folded(2, who > me, True)

    ones = jnp.ones((SUB, 2 * LANES), jnp.bfloat16)
    nt = (((1,), (1,)), ((), ()))

    def pow_bulk(w):
        return pltpu.make_async_remote_copy(
            src_ref=pow_v.at[mw], dst_ref=pow_v.at[mw], send_sem=ps_sem, recv_sem=pr_sem,
            device_id={"width": w}, device_id_type=MESH)

    def bulk_to(k):
        own = jnp.where(mw == 0, 0, jnp.where(mw == 1, nw, mw - 1))
        n = k + jnp.where(k >= own, 1, 0)
        return n + jnp.where(n >= 1, 1, 0)

    def pow_all():
        every = pow_v.at[pl.ds(0, nw - 1)]
        return pltpu.make_async_remote_copy(
            src_ref=every, dst_ref=every, send_sem=ps_sem, recv_sem=pr_sem,
            device_id={"width": other(0, mw)}, device_id_type=MESH)

    def rows_of(b):
        return [pl.ds((b * LANES + j) // seg * pitch + (b * LANES + j) % seg, 2 * SUB) for j in range(0, LANES, 2 * SUB)]

    f16, b16 = jnp.concatenate([f_in] * 2, 0), jnp.concatenate([b_in] * 2, 0)

    def power_stage(carried):
        pending, depth = [], 3

        def store_power(b, res):
            pow_v[mw, pl.ds(b, 1), :] = res[0:1, :LANES]
            pow_v[mw, pl.ds(b + 1, 1), :] = res[0:1, LANES:]
            if b + 2 == NB:
                @pl.when(mw != 1)
                def _():
                    pow_bulk(1).start()

        for b in range(0, NB, 2):
            hi, lo = [], []
            for r in rows_of(b) + rows_of(b + 1):
                st = state_v[r, :] + suf_v[r, :] * b16
                if carried:
                    st = st + pre_v[r, :] * f16
                state_v[r, :] = st
                x = st * st
                h = x.astype(jnp.bfloat16)
                hi.append(h)
                lo.append((x - h.astype(jnp.float32)).astype(jnp.bfloat16))
            both = jnp.concatenate([jnp.concatenate(hi, 0), jnp.concatenate(lo, 0)], 1)
            pending.append((b, lax.dot_general(ones, both, nt, preferred_element_type=jnp.float32)))
            if len(pending) > depth:
                store_power(*pending.pop(0))
        for p in pending:
            store_power(*p)

    @pl.when(me == 0)
    def _():
        power_stage(False)

    @pl.when(me != 0)
    def _():
        power_stage(True)

    for k in range(nw - 2):
        pow_bulk(bulk_to(k)).start()
    @pl.when(mw == 1)
    def _():
        pow_bulk(nw - 1).start()

    gain = jnp.broadcast_to(gain_ref[...], (2 * SUB, C))

    def times_gain(s, _):
        for j in range(0, seg, 2 * SUB):
            r = pl.ds(s * pitch + j, 2 * SUB)
            state_v[r, :] = state_v[r, :] * gain
        return 0

    lax.fori_loop(0, NS, times_gain, 0)

    pow_all().wait_recv()
    sent = leak_v.at[pl.ds(0, (nw - 1) * NB + (ns - 1) * 4)]
    pltpu.make_async_remote_copy(
        src_ref=sent, dst_ref=sent, send_sem=ps_sem, recv_sem=pr_sem,
        device_id={"width": other(0, mw)}, device_id_type=MESH).wait_send()


def close_kernel(ns, nw, seg, groups, state_v, pow_v, out_hbm, out_v, sem):
    T, C = out_v.shape
    NB = T // LANES
    pitch = seg + 4
    total = T * ns

    def rows_of(b):
        return [pl.ds((b * LANES + j) // seg * pitch + (b * LANES + j) % seg, 2 * SUB) for j in range(0, LANES, 2 * SUB)]

    acc = pow_v[0]
    for w in range(1, nw):
        acc = acc + pow_v[w]
    scale = lax.rsqrt(acc * (1.0 / (C * nw * total)) + 1e-6) * total ** -0.5
    top = scale.astype(jnp.bfloat16).astype(jnp.float32)
    parts = [top, scale - top]
    line = lax.broadcasted_iota(jnp.int32, (LANES, LANES), 0)
    spot = lax.broadcasted_iota(jnp.int32, (LANES, LANES), 1) == line
    every_one = jnp.ones((2 * LANES, LANES), jnp.bfloat16)
    across = [scale[h * SUB:(h + 1) * SUB].T for h in range(NB // SUB)]
    def diagonal(b):
        return jnp.concatenate(
            [jnp.where(spot, jnp.broadcast_to(p[b:b + 1], (LANES, LANES)), 0.0).astype(jnp.bfloat16) for p in parts], 1)

    def finish(b, wide):
        for q, r in enumerate(rows_of(b)):
            out_v[pl.ds(b * LANES + q * 2 * SUB, 2 * SUB), :] = (
                state_v[r, :] * wide[q * 2 * SUB:(q + 1) * 2 * SUB]).astype(jnp.bfloat16)

    def by_lanes(b):
        return jnp.broadcast_to(across[b // SUB][:, b % SUB:b % SUB + 1], (LANES, LANES))

    def by_dots(bs):
        wide = jnp.dot(jnp.concatenate([diagonal(b) for b in bs], 0), every_one, preferred_element_type=jnp.float32)
        return [wide[n * LANES:(n + 1) * LANES] for n in range(len(bs))]

    plan, first = [], 0
    for lanes, dots in groups:
        bs = list(range(first, first + lanes + dots))
        plan.append((bs, [by_lanes(b) for b in bs[:lanes]] + (by_dots(bs[lanes:]) if dots else [])))
        first += lanes + dots
    for bs, wides in plan:
        for b, w in zip(bs, wides):
            finish(b, w)
        r = pl.ds(bs[0] * LANES, len(bs) * LANES)
        pltpu.make_async_copy(out_v.at[r], out_hbm.at[r], sem).start()
    pltpu.make_async_copy(out_v, out_hbm, sem).wait()


def per_device(ns, nw, leak_rate, signal_in, norm_gain):
    _, T, C = leak_rate.shape
    seg = 64
    NS = T // seg
    NO = NS // SUB
    pitch = seg + 4
    f32 = jnp.float32
    vmem = pl.BlockSpec(memory_space=pltpu.VMEM)
    hbm = pl.BlockSpec(memory_space=pl.ANY)
    state, power = pl.pallas_call(
        functools.partial(join_kernel, ns, nw, seg),
        out_shape=(pltpu.VMEM((NS * pitch, C), f32), pltpu.VMEM((nw, T // LANES, LANES), f32)),
        in_specs=[hbm, hbm, hbm],
        out_specs=(vmem, vmem),
        scratch_shapes=[
            pltpu.VMEM((1, C), f32),
            pltpu.VMEM((NS * pitch, C), f32),
            pltpu.VMEM((T, C), jnp.bfloat16),
            pltpu.VMEM((NS * pitch, C), f32),
            pltpu.VMEM((NS * pitch, C), f32),
            pltpu.VMEM((NS * pitch, C), f32),
            pltpu.VMEM((4, C), f32),
            pltpu.VMEM((4, ns, C), f32),
            pltpu.SemaphoreType.DMA((NO,)),
            pltpu.SemaphoreType.DMA(()),
            pltpu.SemaphoreType.DMA(()),
            pltpu.SemaphoreType.DMA(()),
        ],
        compiler_params=pltpu.CompilerParams(
            collective_id=0, has_side_effects=True, vmem_limit_bytes=32 * 2 ** 20),
    )(pltpu.with_memory_space_constraint(leak_rate[0], pltpu.HBM),
      pltpu.with_memory_space_constraint(signal_in[0], pltpu.HBM),
      pltpu.with_memory_space_constraint(norm_gain[None], pltpu.HBM))
    out = pl.pallas_call(
        functools.partial(close_kernel, ns, nw, seg, GROUPS),
        out_shape=pltpu.HBM((T, C), jnp.bfloat16),
        in_specs=[vmem, vmem],
        out_specs=hbm,
        scratch_shapes=[pltpu.VMEM((T, C), jnp.bfloat16), pltpu.SemaphoreType.DMA(())],
        compiler_params=pltpu.CompilerParams(vmem_limit_bytes=32 * 2 ** 20),
    )(state, power)
    return out[None]


def solution(mesh):
    return jax.shard_map(
        functools.partial(per_device, mesh.shape["seq"], mesh.shape["width"]),
        mesh=mesh,
        in_specs=(P(None, "seq", "width"), P(None, "seq", "width"), P("width")),
        out_specs=P(None, "seq", "width"),
        check_vma=False,
    )
```

```python
import functools
import math

import jax
import jax.numpy as jnp
from jax import lax
from jax.experimental import pallas as pl
from jax.experimental.pallas import tpu as pltpu
from jax.sharding import PartitionSpec as P

LANES = 128
GROUPS = ((2, 3), (2, 3), (1, 3), (1, 1))
SUB = 8
MESH = pl.DeviceIdType.MESH


def join_kernel(ns, nw, seg, leak_hbm, sig_hbm, gain_hbm, state_v, pow_v, gain_ref, leak_v, sig_v, push_v,
                pre_v, suf_v, own_v, tot_v, in_sem, tr_sem, ps_sem, pr_sem):
    T, C = sig_v.shape
    NS = T // seg
    NO = NS // SUB
    NB = T // LANES
    pitch = seg + 4
    rows = SUB * seg
    total = T * ns
    me = lax.axis_index("seq")
    mw = lax.axis_index("width")

    def load(o):
        r = pl.ds(o * rows, rows)
        yield pltpu.make_async_copy(sig_hbm.at[r], sig_v.at[r], in_sem.at[o])
        for n in range(o * SUB, (o + 1) * SUB):
            yield pltpu.make_async_copy(
                leak_hbm.at[pl.ds(n * seg, seg)], leak_v.at[pl.ds(n * pitch, seg)], in_sem.at[o])

    def loaded(o):
        every = pl.ds(0, rows + rows // 2 + (1 if o == NO - 1 else 0))
        return pltpu.make_async_copy(leak_hbm.at[every], leak_v.at[every], in_sem.at[o])

    for o in range(NO):
        for c in load(o):
            c.start()

    pltpu.make_async_copy(gain_hbm, gain_ref, in_sem.at[NO - 1]).start()

    barrier = pltpu.get_barrier_semaphore()
    for k in sorted(range(1, nw), key=lambda k: abs(min(k, nw - k) - 3 * nw // 8)):
        pl.semaphore_signal(barrier, inc=1, device_id={"width": lax.rem(mw + k, nw)}, device_id_type=MESH)
    for k in sorted(range(1, ns), key=lambda k: abs(min(k, ns - k) - 4)):
        pl.semaphore_signal(barrier, inc=1, device_id={"seq": lax.rem(me + k, ns)}, device_id_type=MESH)

    def at(o, i):
        return pl.ds(o * SUB * pitch + i, SUB, stride=pitch)

    zero = jnp.zeros((SUB, LANES), jnp.float32)
    one = jnp.ones((SUB, LANES), jnp.float32)

    def fill_octet(o):
        def fill(h, _):
            for n in range(SUB // 2):
                n += h * (SUB // 2) + o * SUB
                for j in range(0, seg, 2 * SUB):
                    push_v[pl.ds(n * pitch + j, 2 * SUB), :] = sig_v[
                        pl.ds(pl.multiple_of(n * seg + j, 2 * SUB), 2 * SUB), :].astype(jnp.float32)
            return 0

        lax.fori_loop(0, 2, fill, 0)

    def keep_of(r):
        return jnp.exp2(leak_v[r, :] * (-math.log2(math.e) / total))

    def segment_ends(o):
        half = seg // 2

        def ends_step(i, carry):
            new = []
            for h, (f, b, p) in enumerate(carry):
                r = at(o, i + h * half)
                k = keep_of(r)
                x = push_v[r, :]
                new.append((k * f + x, b + p * x, p * k))
            return tuple(new)

        (f0, b0, p0), (f1, b1, p1) = lax.fori_loop(0, half, ends_step, ((zero, zero, one),) * 2, unroll=16)
        return p1 * f0 + f1, b0 + p0 * b1, p0 * p1

    ends = []
    for o in range(NO):
        loaded(o).wait()
        fill_octet(o)
        ends.append(segment_ends(o))

    def gathered(which):
        return jnp.concatenate([e[which] for e in ends], 0)

    f_end, b_end, p_end = gathered(0), gathered(1), gathered(2)
    row = lax.broadcasted_iota(jnp.int32, (NS, C), 0)

    def shifted(x, d, fill):
        if d > 0:
            return jnp.where(row >= d, pltpu.roll(x, d, 0), fill)
        return jnp.where(row < NS + d, pltpu.roll(x, NS + d, 0), fill)

    pf, ff = p_end, f_end
    pb, bb = p_end, b_end
    d = 1
    while d < NS:
        ff = ff + pf * shifted(ff, d, 0.0)
        pf = pf * shifted(pf, d, 1.0)
        bb = bb + pb * shifted(bb, -d, 0.0)
        pb = pb * shifted(pb, -d, 1.0)
        d *= 2
    own_v[...] = jnp.concatenate(
        [pf[NS - 1:NS], ff[NS - 1:NS], bb[0:1]], 0)
    for n in range(3):
        tot_v[n, pl.ds(me, 1)] = jnp.zeros((1, C), jnp.float32)

    pl.semaphore_wait(barrier, ns + nw - 2)

    def other(k, own):
        return k + jnp.where(k >= own, 1, 0)

    def tot_send(k):
        return pltpu.make_async_remote_copy(
            src_ref=own_v, dst_ref=tot_v.at[:, me], send_sem=ps_sem, recv_sem=tr_sem,
            device_id={"seq": other(k, me)}, device_id_type=MESH)

    def tot_all():
        every = tot_v.at[:, pl.ds(0, ns - 1)]
        return pltpu.make_async_remote_copy(
            src_ref=every, dst_ref=every, send_sem=ps_sem, recv_sem=tr_sem,
            device_id={"seq": other(0, me)}, device_id_type=MESH)

    for k in range(ns - 1):
        tot_send(k).start()

    def octets_of(x):
        return [x[o * SUB:(o + 1) * SUB] for o in range(NO)]

    f_from, p_from = octets_of(shifted(ff, 1, 0.0)), octets_of(shifted(pf, 1, 1.0))
    b_from, q_from = octets_of(shifted(bb, -1, 0.0)), octets_of(shifted(pb, -1, 1.0))

    def ahead(i, carry):
        new = []
        for o, (f, p) in enumerate(carry):
            r = at(o, i)
            k = keep_of(r)
            f = k * f + push_v[r, :]
            p = p * k
            state_v[r, :] = f
            pre_v[r, :] = p
            new.append((f, p))
        return tuple(new)

    lax.fori_loop(0, seg, ahead, tuple(zip(f_from, p_from)), unroll=4)

    def back(n, carry):
        i = seg - 1 - n
        new = []
        for o, (b, q) in enumerate(carry):
            r = at(o, i)
            k = keep_of(r)
            b = k * b + push_v[r, :]
            q = k * q
            state_v[r, :] = state_v[r, :] + b
            suf_v[r, :] = q
            new.append((b, q))
        return tuple(new)

    lax.fori_loop(0, seg, back, tuple(zip(b_from, q_from)), unroll=4)

    tot_all().wait_recv()
    def folded(which, mask, later_first):
        p = jnp.where(mask, tot_v[0], 1.0)
        x = jnp.where(mask, tot_v[which], 0.0)
        n = ns
        while n > 1:
            d = ns // n
            pl_, xl = pltpu.roll(p, ns - d, 0), pltpu.roll(x, ns - d, 0)
            x = x + p * xl if later_first else pl_ * x + xl
            p = p * pl_
            n //= 2
        return jnp.broadcast_to(x[0:1], (SUB, C))

    who = lax.broadcasted_iota(jnp.int32, (ns, C), 0)
    f_in = folded(1, who < me, False)
    b_in = folded(2, who > me, True)

    ones = jnp.ones((SUB, 2 * LANES), jnp.bfloat16)
    nt = (((1,), (1,)), ((), ()))

    def pow_bulk(w):
        return pltpu.make_async_remote_copy(
            src_ref=pow_v.at[mw], dst_ref=pow_v.at[mw], send_sem=ps_sem, recv_sem=pr_sem,
            device_id={"width": w}, device_id_type=MESH)

    def bulk_to(k):
        own = jnp.where(mw == 0, 0, jnp.where(mw == 1, nw, mw - 1))
        n = k + jnp.where(k >= own, 1, 0)
        return n + jnp.where(n >= 1, 1, 0)

    def pow_all():
        every = pow_v.at[pl.ds(0, nw - 1)]
        return pltpu.make_async_remote_copy(
            src_ref=every, dst_ref=every, send_sem=ps_sem, recv_sem=pr_sem,
            device_id={"width": other(0, mw)}, device_id_type=MESH)

    def rows_of(b):
        return [pl.ds((b * LANES + j) // seg * pitch + (b * LANES + j) % seg, 2 * SUB) for j in range(0, LANES, 2 * SUB)]

    f16, b16 = jnp.concatenate([f_in] * 2, 0), jnp.concatenate([b_in] * 2, 0)

    def power_stage(carried):
        pending, depth = [], 3

        def store_power(b, res):
            pow_v[mw, pl.ds(b, 1), :] = res[0:1, :LANES]
            pow_v[mw, pl.ds(b + 1, 1), :] = res[0:1, LANES:]
            if b + 2 == NB:
                @pl.when(mw != 1)
                def _():
                    pow_bulk(1).start()

        for b in range(0, NB, 2):
            hi, lo = [], []
            for r in rows_of(b) + rows_of(b + 1):
                st = state_v[r, :] + suf_v[r, :] * b16
                if carried:
                    st = st + pre_v[r, :] * f16
                state_v[r, :] = st
                x = st * st
                h = x.astype(jnp.bfloat16)
                hi.append(h)
                lo.append((x - h.astype(jnp.float32)).astype(jnp.bfloat16))
            both = jnp.concatenate([jnp.concatenate(hi, 0), jnp.concatenate(lo, 0)], 1)
            pending.append((b, lax.dot_general(ones, both, nt, preferred_element_type=jnp.float32)))
            if len(pending) > depth:
                store_power(*pending.pop(0))
        for p in pending:
            store_power(*p)

    @pl.when(me == 0)
    def _():
        power_stage(False)

    @pl.when(me != 0)
    def _():
        power_stage(True)

    for k in range(nw - 2):
        pow_bulk(bulk_to(k)).start()
    @pl.when(mw == 1)
    def _():
        pow_bulk(nw - 1).start()

    gain = jnp.broadcast_to(gain_ref[...], (2 * SUB, C))

    def times_gain(s, _):
        for j in range(0, seg, 2 * SUB):
            r = pl.ds(s * pitch + j, 2 * SUB)
            state_v[r, :] = state_v[r, :] * gain
        return 0

    lax.fori_loop(0, NS, times_gain, 0)

    pow_all().wait_recv()
    sent = leak_v.at[pl.ds(0, (nw - 1) * NB + (ns - 1) * 3)]
    pltpu.make_async_remote_copy(
        src_ref=sent, dst_ref=sent, send_sem=ps_sem, recv_sem=pr_sem,
        device_id={"width": other(0, mw)}, device_id_type=MESH).wait_send()


def close_kernel(ns, nw, seg, groups, state_v, pow_v, out_hbm, out_v, sem):
    T, C = out_v.shape
    NB = T // LANES
    pitch = seg + 4
    total = T * ns

    def rows_of(b):
        return [pl.ds((b * LANES + j) // seg * pitch + (b * LANES + j) % seg, 2 * SUB) for j in range(0, LANES, 2 * SUB)]

    acc = pow_v[0]
    for w in range(1, nw):
        acc = acc + pow_v[w]
    scale = lax.rsqrt(acc * (1.0 / (C * nw * total)) + 1e-6) * total ** -0.5
    top = scale.astype(jnp.bfloat16).astype(jnp.float32)
    parts = [top, scale - top]
    line = lax.broadcasted_iota(jnp.int32, (LANES, LANES), 0)
    spot = lax.broadcasted_iota(jnp.int32, (LANES, LANES), 1) == line
    every_one = jnp.ones((2 * LANES, LANES), jnp.bfloat16)
    across = [scale[h * SUB:(h + 1) * SUB].T for h in range(NB // SUB)]
    def diagonal(b):
        return jnp.concatenate(
            [jnp.where(spot, jnp.broadcast_to(p[b:b + 1], (LANES, LANES)), 0.0).astype(jnp.bfloat16) for p in parts], 1)

    def finish(b, wide):
        for q, r in enumerate(rows_of(b)):
            out_v[pl.ds(b * LANES + q * 2 * SUB, 2 * SUB), :] = (
                state_v[r, :] * wide[q * 2 * SUB:(q + 1) * 2 * SUB]).astype(jnp.bfloat16)

    def by_lanes(b):
        return jnp.broadcast_to(across[b // SUB][:, b % SUB:b % SUB + 1], (LANES, LANES))

    def by_dots(bs):
        wide = jnp.dot(jnp.concatenate([diagonal(b) for b in bs], 0), every_one, preferred_element_type=jnp.float32)
        return [wide[n * LANES:(n + 1) * LANES] for n in range(len(bs))]

    plan, first = [], 0
    for lanes, dots in groups:
        bs = list(range(first, first + lanes + dots))
        plan.append((bs, [by_lanes(b) for b in bs[:lanes]] + (by_dots(bs[lanes:]) if dots else [])))
        first += lanes + dots
    for bs, wides in plan:
        for b, w in zip(bs, wides):
            finish(b, w)
        r = pl.ds(bs[0] * LANES, len(bs) * LANES)
        pltpu.make_async_copy(out_v.at[r], out_hbm.at[r], sem).start()
    pltpu.make_async_copy(out_v, out_hbm, sem).wait()


def per_device(ns, nw, leak_rate, signal_in, norm_gain):
    _, T, C = leak_rate.shape
    seg = 64
    NS = T // seg
    NO = NS // SUB
    pitch = seg + 4
    f32 = jnp.float32
    vmem = pl.BlockSpec(memory_space=pltpu.VMEM)
    hbm = pl.BlockSpec(memory_space=pl.ANY)
    state, power = pl.pallas_call(
        functools.partial(join_kernel, ns, nw, seg),
        out_shape=(pltpu.VMEM((NS * pitch, C), f32), pltpu.VMEM((nw, T // LANES, LANES), f32)),
        in_specs=[hbm, hbm, hbm],
        out_specs=(vmem, vmem),
        scratch_shapes=[
            pltpu.VMEM((1, C), f32),
            pltpu.VMEM((NS * pitch, C), f32),
            pltpu.VMEM((T, C), jnp.bfloat16),
            pltpu.VMEM((NS * pitch, C), f32),
            pltpu.VMEM((NS * pitch, C), f32),
            pltpu.VMEM((NS * pitch, C), f32),
            pltpu.VMEM((3, C), f32),
            pltpu.VMEM((3, ns, C), f32),
            pltpu.SemaphoreType.DMA((NO,)),
            pltpu.SemaphoreType.DMA(()),
            pltpu.SemaphoreType.DMA(()),
            pltpu.SemaphoreType.DMA(()),
        ],
        compiler_params=pltpu.CompilerParams(
            collective_id=0, has_side_effects=True, vmem_limit_bytes=32 * 2 ** 20),
    )(pltpu.with_memory_space_constraint(leak_rate[0], pltpu.HBM),
      pltpu.with_memory_space_constraint(signal_in[0], pltpu.HBM),
      pltpu.with_memory_space_constraint(norm_gain[None], pltpu.HBM))
    out = pl.pallas_call(
        functools.partial(close_kernel, ns, nw, seg, GROUPS),
        out_shape=pltpu.HBM((T, C), jnp.bfloat16),
        in_specs=[vmem, vmem],
        out_specs=hbm,
        scratch_shapes=[pltpu.VMEM((T, C), jnp.bfloat16), pltpu.SemaphoreType.DMA(())],
        compiler_params=pltpu.CompilerParams(vmem_limit_bytes=32 * 2 ** 20),
    )(state, power)
    return out[None]


def solution(mesh):
    return jax.shard_map(
        functools.partial(per_device, mesh.shape["seq"], mesh.shape["width"]),
        mesh=mesh,
        in_specs=(P(None, "seq", "width"), P(None, "seq", "width"), P("width")),
        out_specs=P(None, "seq", "width"),
        check_vma=False,
    )
```

```python
import functools
import math

import jax
import jax.numpy as jnp
from jax import lax
from jax.experimental import pallas as pl
from jax.experimental.pallas import tpu as pltpu
from jax.sharding import PartitionSpec as P

LANES = 128
GROUPS = ((2, 3), (2, 3), (1, 3), (1, 1))
SUB = 8
MESH = pl.DeviceIdType.MESH


def join_kernel(ns, nw, seg, leak_hbm, sig_hbm, gain_hbm, state_v, pow_v, gain_ref, leak_v, sig_v, push_v,
                pre_v, suf_v, own_v, tot_v, in_sem, tr_sem, ps_sem, pr_sem):
    T, C = sig_v.shape
    NS = T // seg
    NO = NS // SUB
    NB = T // LANES
    pitch = seg + 4
    rows = SUB * seg
    total = T * ns
    me = lax.axis_index("seq")
    mw = lax.axis_index("width")

    def load(o):
        r = pl.ds(o * rows, rows)
        yield pltpu.make_async_copy(sig_hbm.at[r], sig_v.at[r], in_sem.at[o])
        for n in range(o * SUB, (o + 1) * SUB):
            yield pltpu.make_async_copy(
                leak_hbm.at[pl.ds(n * seg, seg)], leak_v.at[pl.ds(n * pitch, seg)], in_sem.at[o])

    def loaded(o):
        every = pl.ds(0, rows + rows // 2 + (1 if o == NO - 1 else 0))
        return pltpu.make_async_copy(leak_hbm.at[every], leak_v.at[every], in_sem.at[o])

    for o in range(NO):
        for c in load(o):
            c.start()

    pltpu.make_async_copy(gain_hbm, gain_ref, in_sem.at[NO - 1]).start()

    barrier = pltpu.get_barrier_semaphore()
    for k in sorted(range(1, nw), key=lambda k: abs(min(k, nw - k) - 3 * nw // 8)):
        pl.semaphore_signal(barrier, inc=1, device_id={"width": lax.rem(mw + k, nw)}, device_id_type=MESH)
    for k in sorted(range(1, ns), key=lambda k: abs(min(k, ns - k) - 4)):
        pl.semaphore_signal(barrier, inc=1, device_id={"seq": lax.rem(me + k, ns)}, device_id_type=MESH)

    def at(o, i):
        return pl.ds(o * SUB * pitch + i, SUB, stride=pitch)

    zero = jnp.zeros((SUB, LANES), jnp.float32)
    one = jnp.ones((SUB, LANES), jnp.float32)

    def fill_octet(o):
        def fill(h, _):
            for n in range(SUB // 2):
                n += h * (SUB // 2) + o * SUB
                for j in range(0, seg, 2 * SUB):
                    push_v[pl.ds(n * pitch + j, 2 * SUB), :] = sig_v[
                        pl.ds(pl.multiple_of(n * seg + j, 2 * SUB), 2 * SUB), :].astype(jnp.float32)
            return 0

        lax.fori_loop(0, 2, fill, 0)

    def keep_of(r):
        return jnp.exp2(leak_v[r, :] * (-math.log2(math.e) / total))

    def segment_ends(o):
        half = seg // 2

        def ends_step(i, carry):
            new = []
            for h, (f, b, p) in enumerate(carry):
                r = at(o, i + h * half)
                k = keep_of(r)
                x = push_v[r, :]
                new.append((k * f + x, b + p * x, p * k))
            return tuple(new)

        (f0, b0, p0), (f1, b1, p1) = lax.fori_loop(0, half, ends_step, ((zero, zero, one),) * 2, unroll=16)
        return p1 * f0 + f1, b0 + p0 * b1, p0 * p1

    ends = []
    for o in range(NO):
        loaded(o).wait()
        fill_octet(o)
        ends.append(segment_ends(o))

    def gathered(which):
        return jnp.concatenate([e[which] for e in ends], 0)

    f_end, b_end, p_end = gathered(0), gathered(1), gathered(2)
    row = lax.broadcasted_iota(jnp.int32, (NS, C), 0)

    def shifted(x, d, fill):
        if d > 0:
            return jnp.where(row >= d, pltpu.roll(x, d, 0), fill)
        return jnp.where(row < NS + d, pltpu.roll(x, NS + d, 0), fill)

    pf, ff = p_end, f_end
    pb, bb = p_end, b_end
    d = 1
    while d < NS:
        ff = ff + pf * shifted(ff, d, 0.0)
        pf = pf * shifted(pf, d, 1.0)
        bb = bb + pb * shifted(bb, -d, 0.0)
        pb = pb * shifted(pb, -d, 1.0)
        d *= 2
    own_v[...] = jnp.concatenate(
        [pf[NS - 1:NS], ff[NS - 1:NS], bb[0:1]], 0)
    for n in range(3):
        tot_v[n, pl.ds(me, 1)] = jnp.zeros((1, C), jnp.float32)

    pl.semaphore_wait(barrier, ns + nw - 2)

    def other(k, own):
        return k + jnp.where(k >= own, 1, 0)

    def tot_send(k):
        return pltpu.make_async_remote_copy(
            src_ref=own_v, dst_ref=tot_v.at[:, me], send_sem=ps_sem, recv_sem=tr_sem,
            device_id={"seq": other(k, me)}, device_id_type=MESH)

    def tot_all():
        every = tot_v.at[:, pl.ds(0, ns - 1)]
        return pltpu.make_async_remote_copy(
            src_ref=every, dst_ref=every, send_sem=ps_sem, recv_sem=tr_sem,
            device_id={"seq": other(0, me)}, device_id_type=MESH)

    for k in range(ns - 1):
        tot_send(k).start()

    def octets_of(x):
        return [x[o * SUB:(o + 1) * SUB] for o in range(NO)]

    f_from, p_from = octets_of(shifted(ff, 1, 0.0)), octets_of(shifted(pf, 1, 1.0))
    b_from, q_from = octets_of(shifted(bb, -1, 0.0)), octets_of(shifted(pb, -1, 1.0))

    def ahead(i, carry):
        new = []
        for o, (f, p) in enumerate(carry):
            r = at(o, i)
            k = keep_of(r)
            f = k * f + push_v[r, :]
            p = p * k
            state_v[r, :] = f
            pre_v[r, :] = p
            new.append((f, p))
        return tuple(new)

    lax.fori_loop(0, seg, ahead, tuple(zip(f_from, p_from)), unroll=4)

    def back(n, carry):
        i = seg - 1 - n
        new = []
        for o, (b, q) in enumerate(carry):
            r = at(o, i)
            k = keep_of(r)
            b = k * b + push_v[r, :]
            q = k * q
            state_v[r, :] = state_v[r, :] + b
            suf_v[r, :] = q
            new.append((b, q))
        return tuple(new)

    lax.fori_loop(0, seg, back, tuple(zip(b_from, q_from)), unroll=4)

    tot_all().wait_recv()
    def folded(which, mask, later_first):
        p = jnp.where(mask, tot_v[0], 1.0)
        x = jnp.where(mask, tot_v[which], 0.0)
        n = ns
        while n > 1:
            d = ns // n
            pl_, xl = pltpu.roll(p, ns - d, 0), pltpu.roll(x, ns - d, 0)
            x = x + p * xl if later_first else pl_ * x + xl
            p = p * pl_
            n //= 2
        return jnp.broadcast_to(x[0:1], (SUB, C))

    who = lax.broadcasted_iota(jnp.int32, (ns, C), 0)
    f_in = folded(1, who < me, False)
    b_in = folded(2, who > me, True)

    ones = jnp.ones((SUB, 2 * LANES), jnp.bfloat16)
    nt = (((1,), (1,)), ((), ()))

    def pow_bulk(w):
        return pltpu.make_async_remote_copy(
            src_ref=pow_v.at[mw], dst_ref=pow_v.at[mw], send_sem=ps_sem, recv_sem=pr_sem,
            device_id={"width": w}, device_id_type=MESH)

    def bulk_to(k):
        own = jnp.where(mw == 0, 0, jnp.where(mw == 1, nw, mw - 1))
        n = k + jnp.where(k >= own, 1, 0)
        return n + jnp.where(n >= 1, 1, 0)

    def pow_all():
        every = pow_v.at[pl.ds(0, nw - 1)]
        return pltpu.make_async_remote_copy(
            src_ref=every, dst_ref=every, send_sem=ps_sem, recv_sem=pr_sem,
            device_id={"width": other(0, mw)}, device_id_type=MESH)

    def rows_of(b):
        return [pl.ds((b * LANES + j) // seg * pitch + (b * LANES + j) % seg, 2 * SUB) for j in range(0, LANES, 2 * SUB)]

    f16, b16 = jnp.concatenate([f_in] * 2, 0), jnp.concatenate([b_in] * 2, 0)

    def power_stage(carried):
        pending, depth = [], 3

        def store_power(b, res):
            pow_v[mw, pl.ds(b, 1), :] = res[0:1, :LANES]
            pow_v[mw, pl.ds(b + 1, 1), :] = res[0:1, LANES:]
            if b + 2 == NB:
                @pl.when(mw != 1)
                def _():
                    pow_bulk(1).start()

        for b in range(0, NB, 2):
            hi, lo = [], []
            for r in rows_of(b) + rows_of(b + 1):
                st = state_v[r, :] + suf_v[r, :] * b16
                if carried:
                    st = st + pre_v[r, :] * f16
                state_v[r, :] = st
                x = st * st
                h = x.astype(jnp.bfloat16)
                hi.append(h)
                lo.append((x - h.astype(jnp.float32)).astype(jnp.bfloat16))
            both = jnp.concatenate([jnp.concatenate(hi, 0), jnp.concatenate(lo, 0)], 1)
            pending.append((b, lax.dot_general(ones, both, nt, preferred_element_type=jnp.float32)))
            if len(pending) > depth:
                store_power(*pending.pop(0))
        for p in pending:
            store_power(*p)

    @pl.when(me == 0)
    def _():
        power_stage(False)

    @pl.when(me != 0)
    def _():
        power_stage(True)

    for k in range(nw - 2):
        pow_bulk(bulk_to(k)).start()
    @pl.when(mw == 1)
    def _():
        pow_bulk(nw - 1).start()

    gain = jnp.broadcast_to(gain_ref[...], (2 * SUB, C))

    def times_gain(s, _):
        for j in range(0, seg, 2 * SUB):
            r = pl.ds(s * pitch + j, 2 * SUB)
            state_v[r, :] = state_v[r, :] * gain
        return 0

    lax.fori_loop(0, NS, times_gain, 0)

    pow_all().wait_recv()
    sent = leak_v.at[pl.ds(0, (nw - 1) * NB + (ns - 1) * 3)]
    pltpu.make_async_remote_copy(
        src_ref=sent, dst_ref=sent, send_sem=ps_sem, recv_sem=pr_sem,
        device_id={"width": other(0, mw)}, device_id_type=MESH).wait_send()


def close_kernel(ns, nw, seg, groups, state_v, pow_v, out_hbm, out_v, sem):
    T, C = out_v.shape
    NB = T // LANES
    pitch = seg + 4
    total = T * ns

    def rows_of(b):
        return [pl.ds((b * LANES + j) // seg * pitch + (b * LANES + j) % seg, 2 * SUB) for j in range(0, LANES, 2 * SUB)]

    sums = [pow_v[w] for w in range(nw)]
    while len(sums) > 1:
        sums = [sum(sums[n:n + 2][1:], sums[n]) for n in range(0, len(sums), 2)]
    acc = sums[0]
    scale = lax.rsqrt(acc * (1.0 / (C * nw * total)) + 1e-6) * total ** -0.5
    top = scale.astype(jnp.bfloat16).astype(jnp.float32)
    parts = [top, scale - top]
    line = lax.broadcasted_iota(jnp.int32, (LANES, LANES), 0)
    spot = lax.broadcasted_iota(jnp.int32, (LANES, LANES), 1) == line
    every_one = jnp.ones((2 * LANES, LANES), jnp.bfloat16)
    across = [scale[h * SUB:(h + 1) * SUB].T for h in range(NB // SUB)]
    def diagonal(b):
        return jnp.concatenate(
            [jnp.where(spot, jnp.broadcast_to(p[b:b + 1], (LANES, LANES)), 0.0).astype(jnp.bfloat16) for p in parts], 1)

    def finish(b, wide):
        for q, r in enumerate(rows_of(b)):
            out_v[pl.ds(b * LANES + q * 2 * SUB, 2 * SUB), :] = (
                state_v[r, :] * wide[q * 2 * SUB:(q + 1) * 2 * SUB]).astype(jnp.bfloat16)

    def by_lanes(b):
        return jnp.broadcast_to(across[b // SUB][:, b % SUB:b % SUB + 1], (LANES, LANES))

    def by_dots(bs):
        wide = jnp.dot(jnp.concatenate([diagonal(b) for b in bs], 0), every_one, preferred_element_type=jnp.float32)
        return [wide[n * LANES:(n + 1) * LANES] for n in range(len(bs))]

    plan, first = [], 0
    for lanes, dots in groups:
        bs = list(range(first, first + lanes + dots))
        plan.append((bs, [by_lanes(b) for b in bs[:lanes]] + (by_dots(bs[lanes:]) if dots else [])))
        first += lanes + dots
    for bs, wides in plan:
        for b, w in zip(bs, wides):
            finish(b, w)
        r = pl.ds(bs[0] * LANES, len(bs) * LANES)
        pltpu.make_async_copy(out_v.at[r], out_hbm.at[r], sem).start()
    pltpu.make_async_copy(out_v, out_hbm, sem).wait()


def per_device(ns, nw, leak_rate, signal_in, norm_gain):
    _, T, C = leak_rate.shape
    seg = 64
    NS = T // seg
    NO = NS // SUB
    pitch = seg + 4
    f32 = jnp.float32
    vmem = pl.BlockSpec(memory_space=pltpu.VMEM)
    hbm = pl.BlockSpec(memory_space=pl.ANY)
    state, power = pl.pallas_call(
        functools.partial(join_kernel, ns, nw, seg),
        out_shape=(pltpu.VMEM((NS * pitch, C), f32), pltpu.VMEM((nw, T // LANES, LANES), f32)),
        in_specs=[hbm, hbm, hbm],
        out_specs=(vmem, vmem),
        scratch_shapes=[
            pltpu.VMEM((1, C), f32),
            pltpu.VMEM((NS * pitch, C), f32),
            pltpu.VMEM((T, C), jnp.bfloat16),
            pltpu.VMEM((NS * pitch, C), f32),
            pltpu.VMEM((NS * pitch, C), f32),
            pltpu.VMEM((NS * pitch, C), f32),
            pltpu.VMEM((3, C), f32),
            pltpu.VMEM((3, ns, C), f32),
            pltpu.SemaphoreType.DMA((NO,)),
            pltpu.SemaphoreType.DMA(()),
            pltpu.SemaphoreType.DMA(()),
            pltpu.SemaphoreType.DMA(()),
        ],
        compiler_params=pltpu.CompilerParams(
            collective_id=0, has_side_effects=True, vmem_limit_bytes=32 * 2 ** 20),
    )(pltpu.with_memory_space_constraint(leak_rate[0], pltpu.HBM),
      pltpu.with_memory_space_constraint(signal_in[0], pltpu.HBM),
      pltpu.with_memory_space_constraint(norm_gain[None], pltpu.HBM))
    out = pl.pallas_call(
        functools.partial(close_kernel, ns, nw, seg, GROUPS),
        out_shape=pltpu.HBM((T, C), jnp.bfloat16),
        in_specs=[vmem, vmem],
        out_specs=hbm,
        scratch_shapes=[pltpu.VMEM((T, C), jnp.bfloat16), pltpu.SemaphoreType.DMA(())],
        compiler_params=pltpu.CompilerParams(vmem_limit_bytes=32 * 2 ** 20),
    )(state, power)
    return out[None]


def solution(mesh):
    return jax.shard_map(
        functools.partial(per_device, mesh.shape["seq"], mesh.shape["width"]),
        mesh=mesh,
        in_specs=(P(None, "seq", "width"), P(None, "seq", "width"), P("width")),
        out_specs=P(None, "seq", "width"),
        check_vma=False,
    )
```
